128 devices in a mesh: rep: 8 (over z, y_lo), fsdp: 16 (over y_hi, x, core).
Axes of the slice: x: 4, y: 4 (y_hi: 2, y_lo: 2; y = y_hi * 2 + y_lo), z: 4, core: 2. Of those that a mesh axis runs over, the one named last changes fastest.
Arguments:
- tokens: bfloat16 [65536, 2048], P(('rep', 'fsdp')), may hold values from -6 to 6
- norm_gain: float32 [2048], replicated, may hold values from 0.5 to 1.5
- outer_params: float32 [2, 2048, 4096], P(None, 'fsdp'), may hold values from -6 to 6
- momentum: float32 [2, 2048, 4096], P(None, 'fsdp'), may hold values from -6 to 6
- deltas: bfloat16 [8, 2, 2048, 4096], P('rep', None, 'fsdp'), may hold values from -6 to 6
Outputs:
- new_params: float32 [2, 2048, 4096], P(None, 'fsdp')
- new_momentum: float32 [2, 2048, 4096], P(None, 'fsdp')
- hidden: bfloat16 [65536, 4096], P(('rep', 'fsdp'))
The draws below stay inside these ranges and needn't reach their ends.
All inputs are finite; a program needn't handle non-finite values.
Results may differ from the reference program's by a relative error of at most 0.01.
Values may be sent and summed in bfloat16 or wider, within the bound.
A program may use at most 192 MiB of HBM per device.

```python
import math
import jax
import jax.numpy as jnp
from jax import lax

D = 2048
FF = 4096
TOKENS = 65536
N_REP = 8


def block_levels(stream_key, shape, split, least, largest):
    def one(position, blocks):
        heights = jax.random.uniform(jax.random.fold_in(jax.random.fold_in(stream_key, 6), position), (blocks,), jnp.float32, least / len(split), largest / len(split))
        return jnp.repeat(jnp.exp(heights), shape[position] // blocks).reshape((-1,) + (1,) * (len(shape) - position - 1))

    loudness = one(*split[0])
    for cut in split[1:]:
        loudness = loudness * one(*cut)
    return loudness


def normal_values(stream_key, dims, deviation, most, pieces=(), held_as=jnp.bfloat16):
    values = jax.random.normal(stream_key, dims, jnp.float32) * deviation
    if len(pieces) > 0:
        values = block_levels(stream_key, dims, pieces, -0.22, 0.18) * values
    return jnp.clip(values, min=-most, max=most).astype(held_as)


def setup_inputs(seed: int = 0) -> dict:
    key_list = jax.random.split(jax.random.key(seed), 6)
    return {
        "tokens": normal_values(key_list[0], (TOKENS, D), 1.0, 6.0, ((0, 128),)),
        "norm_gain": jnp.clip(1.0 + 0.1 * jax.random.normal(key_list[1], (D,), jnp.float32), 0.5, 1.5),
        "outer_params": normal_values(key_list[2], (2, D, FF), 1.0, 6.0, ((1, 16),), jnp.float32),
        "momentum": normal_values(key_list[3], (2, D, FF), 0.5, 6.0, ((1, 16),), jnp.float32),
        "deltas": normal_values(key_list[4], (N_REP, 2, D, FF), 0.5, 6.0, ((0, 8), (2, 16))),
    }


EPS = 1e-05
MU = 0.9
RATE = 0.7

def reference(tokens, norm_gain, outer_params, momentum, deltas):
    total = jnp.zeros(outer_params.shape, jnp.float32)
    for group in range(N_REP):
        total = total + deltas[group].astype(jnp.float32)
    outer_grad = total / N_REP
    new_momentum = MU * momentum + outer_grad
    new_params = outer_params - RATE * (outer_grad + MU * new_momentum)
    weights = new_params.astype(jnp.bfloat16)
    values = tokens.astype(jnp.float32)
    scale_rows = lax.rsqrt(lax.optimization_barrier(jnp.mean(values * values, axis=-1, keepdims=True)) + EPS)
    normed = (values * scale_rows * norm_gain).astype(jnp.bfloat16)
    factor = 1.0 / math.sqrt(D)
    gate = jnp.dot(normed, weights[0], preferred_element_type=jnp.float32) * factor
    up = jnp.dot(normed, weights[1], preferred_element_type=jnp.float32) * factor
    hidden = (jax.nn.silu(gate) * up).astype(jnp.bfloat16)
    return (new_params, new_momentum, hidden)
```

```python
import functools
import math

import jax
import jax.numpy as jnp
from jax import lax
from jax.experimental import pallas as pl
from jax.experimental.pallas import tpu as pltpu
from jax.sharding import PartitionSpec as P

EPS = 1e-05
MU = 0.9
RATE = 0.7
MESH = pl.DeviceIdType.MESH
ALL = slice(None)

ORDERS = {"x": ("y", "z", "x"), "y": ("z", "x", "y"), "z": ("x", "y", "z")}
SETS = ({"x": (0, 6), "y": (6, 5), "z": (11, 5)},)
UNITS = 16
LANES = 128
HALF = 2048


def advance(params, moment, outer_grad):
    moment_next = MU * moment + outer_grad
    params_next = params - RATE * (outer_grad + MU * moment_next)
    return (params_next, moment_next)


def kernel(
    tokens, gain, params, moment, deltas, hidden, grads,
    wts, tok, normed, got, pbuf, mbuf, gsum, stage, hbuf,
    loc, rs_s, rs_r, tk_s, tk_r, dd_s, dd_r, p1_s, p1_r, p2_s, p2_r, p3_s, p3_r,
    g_s, g_r, h_l, h_s, h_r,
):
    rep = lax.axis_index("rep")
    fsdp = lax.axis_index("fsdp")
    z, yl = rep // 2, rep % 2
    yh, x, core = fsdp // 8, (fsdp // 2) % 4, fsdp % 2
    y = yh * 2 + yl
    here = {"x": x, "y": y, "z": z}

    def device(at, c):
        return (at["z"] * 2 + at["y"] % 2, (at["y"] // 2) * 8 + at["x"] * 2 + c)

    def shifted(axis, step):
        return {**here, axis: (here[axis] + step + 4) % 4}

    partner = (rep, yh * 8 + x * 2 + (1 - core))
    ydev = device({**here, "y": yh * 2 + (1 - yl)}, core)

    def rep_peer(k):
        return ((z + k // 2) % 4) * 2 + (yl + k % 2) % 2

    barrier = pltpu.get_barrier_semaphore()
    greet = [device(shifted(a, d), core) for a in "xyz" for d in (1, -1)]
    greet += [partner] + [(rep_peer(k), fsdp) for k in range(1, 8)]
    for who in greet:
        pl.semaphore_signal(barrier, inc=1, device_id=who, device_id_type=MESH)

    locals_ = [
        pltpu.make_async_copy(tokens, tok.at[0], loc.at[0]),
        pltpu.make_async_copy(deltas.at[:, rep], got.at[0], loc.at[1]),
        pltpu.make_async_copy(params.at[:, rep], pbuf, loc.at[2]),
        pltpu.make_async_copy(moment.at[:, rep], mbuf, loc.at[3]),
    ]
    for c in locals_:
        c.start()
    pl.semaphore_wait(barrier, len(greet))

    sent = []

    def remote(src, dst, s, r, who):
        return pltpu.make_async_remote_copy(
            src_ref=src, dst_ref=dst, send_sem=s, recv_sem=r, device_id=who, device_id_type=MESH
        )

    def send(src, dst, s, r, who):
        c = remote(src, dst, s, r, who)
        c.start()
        sent.append(c)

    for k in (4, 5, 2, 3, 6, 7, 1):
        q = rep_peer(k)
        send(deltas.at[:, q], got.at[k], rs_s.at[k], rs_r.at[k], (q, fsdp))
    send(tokens, tok.at[1], tk_s, tk_r, partner)

    locals_[0].wait()
    remote(tokens, tok.at[1], tk_s, tk_r, partner).wait_recv()
    chunk = 32

    def norm_step(i, carry):
        rows = pl.ds(pl.multiple_of((i % 16) * chunk, chunk), chunk)
        v = tok[i // 16, rows, :].astype(jnp.float32)
        scale = lax.rsqrt(jnp.mean(v * v, axis=-1, keepdims=True) + EPS)
        normed[pl.ds(pl.multiple_of(i * chunk, chunk), chunk), :] = (v * scale * gain[...]).astype(jnp.bfloat16)
        return carry

    lax.fori_loop(0, 1024 // chunk, norm_step, 0)

    for c in locals_[1:]:
        c.wait()
    for k in range(1, 8):
        remote(got.at[k], got.at[k], rs_s.at[k], rs_r.at[k], partner).wait_recv()

    def update_step(j, carry):
        for other in (True, False):
            col = ((1 - core) if other else core) * HALF + j * LANES
            cols = pl.ds(pl.multiple_of(col, LANES), LANES)
            for mat in range(2):
                acc = got[0, mat, :, cols].astype(jnp.float32)
                for k in range(1, 8):
                    acc = acc + got[k, mat, :, cols].astype(jnp.float32)
                g = acc * (1.0 / 8)
                gsum[mat, z, yl, :, cols] = g.astype(jnp.bfloat16)
                new, _ = advance(pbuf[mat, :, cols], mbuf[mat, :, cols], g)
                w = new.astype(jnp.bfloat16)
                lanes = pl.ds(mat * LANES, LANES)
                if other:
                    stage[j, :, lanes] = w
                else:
                    wts[j, yh, x, core, z, yl, :, lanes] = w
        return carry

    lax.fori_loop(0, UNITS, update_step, 0)
    send(stage, wts.at[:, yh, x, core, z, yl], dd_s, dd_r, partner)
    remote(stage, wts.at[:, yh, x, 1 - core, z, yl], dd_s, dd_r, partner).wait_recv()

    def region(us, at, half=ALL):
        ax, ay, az = at["x"], at["y"], at["z"]
        fx = ALL if ax is None else ax
        fz = ALL if az is None else az
        fh, fl = (ALL, ALL) if ay is None else (ay // 2, ay % 2)
        return wts.at[us, fh, fx, half, fz, fl]

    class Ring:
        def __init__(self, us, order, phase, s, r):
            self.us, self.axis, self.s, self.r = us, order[phase], s, r
            self.base = {a: (None if a in order[:phase] else here[a]) for a in "xyz"}
            self.to = [device(shifted(self.axis, d), core) for d in (1, -1)]

        def at(self, step):
            return {**self.base, self.axis: (here[self.axis] + step + 4) % 4}

        def start(self):
            own = region(self.us, self.at(0))
            for d in range(2):
                send(own, own, self.s.at[d], self.r.at[d], self.to[d])

        def forward(self):
            for d in range(2):
                back = self.at(-1 if d == 0 else 1)
                full = region(self.us, back)
                remote(full, full, self.s.at[d], self.r.at[d], self.to[d]).wait_recv()
                part = region(self.us, back, d)
                send(part, part, self.s.at[2 + d], self.r.at[2 + d], self.to[d])

        def finish(self):
            for d in range(2):
                far = region(self.us, self.at(2), d)
                remote(far, far, self.s.at[2 + d], self.r.at[2 + d], self.to[d]).wait_recv()

    names = ("x", "y", "z")
    parts = SETS[0]

    def rings(phase, s, r):
        return [
            Ring(pl.ds(parts[n][0], parts[n][1]), ORDERS[n], phase, s.at[i], r.at[i])
            for i, n in enumerate(names)
        ]

    for phase, s, r in ((0, p1_s, p1_r), (1, p2_s, p2_r)):
        group = rings(phase, s, r)
        for step in ("start", "forward", "finish"):
            for ring in group:
                getattr(ring, step)()
        if phase == 0:
            own = gsum.at[:, z, yl]
            send(own, own, g_s.at[4], g_r.at[4], ydev)

    factor = 1.0 / math.sqrt(2048)

    def compute(u):
        def rows_step(m, carry):
            w = wts[u].reshape(2048, 2 * LANES)
            rows = pl.ds(pl.multiple_of(m * 512, 512), 512)
            out = jnp.dot(normed[rows, :], w, preferred_element_type=jnp.float32)
            gate = out[:, :LANES] * factor
            up = out[:, LANES:] * factor
            hbuf[u, m] = ((gate / (1.0 + jnp.exp(-gate))) * up).astype(jnp.bfloat16)
            return carry

        lax.fori_loop(0, 2, rows_step, 0)

    def hidden_cols(c, u):
        return hidden.at[:, pl.ds(pl.multiple_of(c * HALF + u * LANES, LANES), LANES)]

    copies = []

    def emit(u):
        c = pltpu.make_async_copy(hbuf.at[u, 0], hidden_cols(core, u), h_l.at[u])
        c.start()
        copies.append(c)
        send(hbuf.at[u, 1], hidden_cols(core, u), h_s.at[u], h_r.at[u], partner)

    rounds = []
    for k in range(max(parts[n][1] for n in names)):
        us = [(n, parts[n][0] + k) for n in names if k < parts[n][1]]
        rounds.append(
            ([Ring(pl.ds(u, 1), ORDERS[n], 2, p3_s.at[u], p3_r.at[u]) for n, u in us], [u for _, u in us])
        )

    def g_region(step):
        return gsum.at[:, (z + step + 4) % 4]

    zto = [device(shifted("z", d), core) for d in (1, -1)]
    for ring in rounds[0][0]:
        ring.start()
    for k in range(len(rounds)):
        if k + 1 < len(rounds):
            for ring in rounds[k + 1][0]:
                ring.start()
        if k == 0:
            far = gsum.at[:, z, 1 - yl]
            remote(far, far, g_s.at[4], g_r.at[4], ydev).wait_recv()
            for d in range(2):
                send(g_region(0), g_region(0), g_s.at[d], g_r.at[d], zto[d])
        if k == 2:
            for d in range(2):
                back = g_region(-1 if d == 0 else 1)
                remote(back, back, g_s.at[d], g_r.at[d], zto[d]).wait_recv()
                part = gsum.at[:, (z + (3 if d == 0 else 1)) % 4, d]
                send(part, part, g_s.at[2 + d], g_r.at[2 + d], zto[d])
        for ring in rounds[k][0]:
            ring.forward()
        if k >= 1:
            for ring, u in zip(*rounds[k - 1]):
                ring.finish()
                compute(u)
            for u in rounds[k - 1][1]:
                emit(u)
    for d in range(2):
        far = gsum.at[:, (z + 2) % 4, d]
        remote(far, far, g_s.at[2 + d], g_r.at[2 + d], zto[d]).wait_recv()
    out = pltpu.make_async_copy(gsum, grads, loc.at[4])
    out.start()
    for ring, u in zip(*rounds[-1]):
        ring.finish()
        compute(u)
    for u in rounds[-1][1]:
        emit(u)
    out.wait()
    for c in copies:
        c.wait()
    for u in range(UNITS):
        remote(hbuf.at[u, 1], hidden_cols(1 - core, u), h_s.at[u], h_r.at[u], partner).wait_recv()
    for c in sent:
        c.wait_send()


def body(tokens, norm_gain, outer_params, momentum, deltas):
    bf16, f32 = jnp.bfloat16, jnp.float32
    hbm = pl.BlockSpec(memory_space=pl.ANY)
    dma = pltpu.SemaphoreType.DMA
    vmem = pltpu.VMEM
    hidden, grads = pl.pallas_call(
        kernel,
        out_shape=(
            jax.ShapeDtypeStruct((512, 4096), bf16),
            jax.ShapeDtypeStruct((2, 4, 2, 16, 4096), bf16),
        ),
        in_specs=[hbm, pl.BlockSpec(memory_space=pltpu.VMEM), hbm, hbm, hbm],
        out_specs=(hbm, hbm),
        scratch_shapes=[
            vmem((UNITS, 2, 4, 2, 4, 2, 16, 2 * LANES), bf16),
            vmem((2, 512, 2048), bf16),
            vmem((1024, 2048), bf16),
            vmem((8, 2, 16, 4096), bf16),
            vmem((2, 16, 4096), f32),
            vmem((2, 16, 4096), f32),
            vmem((2, 4, 2, 16, 4096), bf16),
            vmem((UNITS, 16, 2 * LANES), bf16),
            vmem((UNITS, 2, 512, LANES), bf16),
            dma((5,)),
            dma((8,)), dma((8,)),
            dma, dma,
            dma, dma,
            dma((3, 4)), dma((3, 4)),
            dma((3, 4)), dma((3, 4)),
            dma((UNITS, 4)), dma((UNITS, 4)),
            dma((5,)), dma((5,)),
            dma((UNITS,)), dma((UNITS,)), dma((UNITS,)),
        ],
        compiler_params=pltpu.CompilerParams(
            collective_id=0, has_side_effects=True, vmem_limit_bytes=62 * 1024 * 1024
        ),
        name="outer_round",
    )(
        tokens,
        norm_gain.reshape(1, 2048),
        outer_params.reshape(2, 8, 16, 4096),
        momentum.reshape(2, 8, 16, 4096),
        deltas.reshape(2, 8, 16, 4096),
    )
    outer_grad = grads.reshape(2, 128, 4096).astype(f32)
    new_params, new_momentum = advance(outer_params, momentum, outer_grad)
    return (new_params, new_momentum, hidden)


def solution(mesh):
    in_specs = (
        P(("rep", "fsdp"), None),
        P(),
        P(None, "fsdp", None),
        P(None, "fsdp", None),
        P("rep", None, "fsdp", None),
    )
    out_specs = (P(None, "fsdp", None), P(None, "fsdp", None), P(("rep", "fsdp"), None))
    return jax.shard_map(body, mesh=mesh, in_specs=in_specs, out_specs=out_specs, check_vma=False)
```

```python
import math

import jax
import jax.numpy as jnp
from jax import lax
from jax.experimental import pallas as pl
from jax.experimental.pallas import tpu as pltpu
from jax.sharding import PartitionSpec as P

EPS = 1e-05
MU = 0.9
RATE = 0.7
MESH = pl.DeviceIdType.MESH
ALL = slice(None)
UNITS = 16
LANES = 128
HALF = 2048

ORDERS = {'x': ('y', 'z', 'x'), 'y': ('z', 'x', 'y'), 'z': ('x', 'y', 'z'), 'g': ('z', 'z', 'z', 'z')}
SPANS = ((0, 4), (4, 5), (9, 2), (11, 5))
PIECES = 2
NORMS = 4
PLAN = (
    ('rs', 0), ('rs', 1), ('norm', 0), ('norm', 1),
    ('norm', 2), ('norm', 3), ('rs2', 0), ('rs', 2),
    ('rs2', 1), ('rs', 3), ('upd', 0), ('rs2', 2),
    ('dd', 0), ('st', 0, 'z', 2, 2), ('st', 0, 'x', 0, 2), ('upd', 1),
    ('fw', 0, 'z', 2, 2), ('dd', 1), ('st', 0, 'z', 8, 1), ('st', 0, 'x', 4, 2),
    ('st', 0, 'y', 6, 2), ('fw', 0, 'x', 0, 2), ('rs2', 3), ('upd', 2),
    ('fi', 0, 'z', 2, 2), ('st', 1, 'z', 2, 1), ('st', 1, 'z', 3, 1), ('fw', 0, 'z', 8, 1),
    ('fw', 0, 'y', 6, 2), ('fw', 0, 'x', 4, 2), ('fi', 0, 'x', 0, 2), ('st', 1, 'x', 0, 1),
    ('st', 1, 'x', 1, 1), ('dd', 2), ('st', 0, 'y', 9, 2), ('fi', 0, 'z', 8, 1),
    ('st', 1, 'z', 8, 1), ('upd', 3), ('gy0',), ('fi', 0, 'y', 6, 2),
    ('st', 1, 'y', 6, 1), ('st', 1, 'y', 7, 1), ('fw', 1, 'x', 0, 1), ('fi', 0, 'x', 4, 2),
    ('st', 1, 'x', 4, 1), ('st', 1, 'x', 5, 1), ('dd', 3), ('st', 0, 'z', 15, 1),
    ('st', 0, 'y', 13, 2), ('fw', 1, 'x', 1, 1), ('fw', 1, 'z', 2, 1), ('fw', 0, 'y', 9, 2),
    ('fw', 1, 'y', 6, 1), ('fw', 1, 'z', 3, 1), ('fi', 1, 'x', 0, 1), ('st', 2, 'x', 0, 1),
    ('fw', 1, 'z', 8, 1), ('st', 0, 'x', 11, 2), ('fw', 1, 'x', 4, 1), ('fi', 1, 'y', 6, 1),
    ('fw', 0, 'z', 15, 1), ('fw', 1, 'y', 7, 1), ('st', 2, 'y', 6, 1), ('fw', 1, 'x', 5, 1),
    ('fw', 0, 'y', 13, 2), ('fi', 1, 'x', 1, 1), ('st', 2, 'x', 1, 1), ('fi', 0, 'y', 9, 2),
    ('gy1',), ('st', 3, 'g', 0, 1), ('fi', 1, 'x', 4, 1), ('fi', 1, 'z', 2, 1),
    ('fi', 1, 'x', 5, 1), ('fi', 1, 'z', 3, 1), ('fi', 0, 'y', 13, 2), ('fi', 1, 'z', 8, 1),
    ('st', 2, 'z', 2, 1), ('fw', 0, 'x', 11, 2), ('fi', 0, 'z', 15, 1), ('st', 1, 'z', 15, 1),
    ('fi', 1, 'y', 7, 1), ('st', 1, 'y', 9, 1), ('st', 2, 'y', 7, 1), ('st', 1, 'y', 10, 1),
    ('st', 1, 'y', 13, 1), ('st', 2, 'z', 3, 1), ('st', 1, 'y', 14, 1), ('fi', 0, 'x', 11, 2),
    ('fw', 2, 'x', 0, 1), ('fw', 2, 'y', 6, 1), ('fw', 1, 'y', 9, 1), ('fw', 1, 'z', 15, 1),
    ('fw', 1, 'y', 10, 1), ('st', 1, 'x', 11, 1), ('fw', 1, 'y', 13, 1), ('fw', 1, 'y', 14, 1),
    ('fw', 2, 'x', 1, 1), ('st', 1, 'x', 12, 1), ('fw', 2, 'y', 7, 1), ('fw', 2, 'z', 2, 1),
    ('fi', 2, 'x', 0, 1), ('st', 2, 'x', 4, 1), ('mm', 0), ('em', 0),
    ('st', 2, 'z', 8, 1), ('fi', 1, 'z', 15, 1), ('fi', 1, 'y', 9, 1), ('st', 2, 'y', 9, 1),
    ('fi', 1, 'y', 10, 1), ('fi', 2, 'y', 6, 1), ('fi', 1, 'y', 13, 1), ('mm', 6),
    ('em', 6), ('st', 2, 'y', 10, 1), ('fi', 1, 'y', 14, 1), ('fi', 2, 'y', 7, 1),
    ('mm', 7), ('em', 7), ('st', 2, 'x', 5, 1), ('fi', 2, 'x', 1, 1),
    ('mm', 1), ('em', 1), ('fw', 1, 'x', 11, 1), ('fw', 1, 'x', 12, 1),
    ('fi', 2, 'z', 2, 1), ('mm', 2), ('em', 2), ('fw', 2, 'z', 3, 1),
    ('fw', 2, 'y', 9, 1), ('fw', 2, 'x', 4, 1), ('st', 2, 'z', 15, 1), ('st', 2, 'y', 13, 1),
    ('fi', 1, 'x', 11, 1), ('fi', 1, 'x', 12, 1), ('st', 2, 'x', 11, 1), ('fi', 2, 'z', 3, 1),
    ('fw', 2, 'z', 8, 1), ('mm', 3), ('em', 3), ('fw', 2, 'y', 10, 1),
    ('fi', 2, 'y', 9, 1), ('mm', 9), ('em', 9), ('fw', 2, 'x', 5, 1),
    ('fw', 3, 'g', 0, 1), ('fi', 2, 'x', 4, 1), ('mm', 4), ('em', 4),
    ('st', 2, 'y', 14, 1), ('fw', 2, 'z', 15, 1), ('st', 2, 'x', 12, 1), ('fi', 2, 'z', 8, 1),
    ('st', 3, 'g', 1, 1), ('mm', 8), ('em', 8), ('fw', 2, 'y', 13, 1),
    ('fi', 2, 'y', 10, 1), ('mm', 10), ('em', 10), ('fw', 2, 'x', 11, 1),
    ('fi', 3, 'g', 0, 1), ('fi', 2, 'x', 5, 1), ('mm', 5), ('em', 5),
    ('fi', 2, 'z', 15, 1), ('mm', 15), ('em', 15), ('fw', 2, 'y', 14, 1),
    ('fw', 2, 'x', 12, 1), ('fi', 2, 'y', 13, 1), ('mm', 13), ('em', 13),
    ('fw', 3, 'g', 1, 1), ('fi', 2, 'x', 11, 1), ('mm', 11), ('em', 11),
    ('fi', 2, 'y', 14, 1), ('mm', 14), ('em', 14), ('fi', 2, 'x', 12, 1),
    ('mm', 12), ('em', 12), ('fi', 3, 'g', 1, 1),
)


def advance(params, moment, outer_grad):
    moment_next = MU * moment + outer_grad
    params_next = params - RATE * (outer_grad + MU * moment_next)
    return (params_next, moment_next)


def kernel(
    tokens, gain, params, moment, deltas, hidden, grads,
    wts, tok, normed, own0, own1, ry0, rz0, rz1, ry1, pz0, pz1, pbuf, mbuf, gsum, stage, hbuf,
    loc, a_s, a_r, b_s, b_r, tk_s, tk_r, dd_s, dd_r, ring_s, ring_r, gy_s, gy_r, h_l, h_s, h_r,
):
    bf16, f32 = jnp.bfloat16, jnp.float32
    rep = lax.axis_index("rep")
    fsdp = lax.axis_index("fsdp")
    z, yl = rep // 2, rep % 2
    yh, x, core = fsdp // 8, (fsdp // 2) % 4, fsdp % 2
    here = {"x": x, "y": yh * 2 + yl, "z": z}

    def device(at):
        return (at["z"] * 2 + at["y"] % 2, (at["y"] // 2) * 8 + at["x"] * 2 + core)

    def shifted(axis, step):
        return {**here, axis: (here[axis] + step + 4) % 4}

    partner = (rep, yh * 8 + x * 2 + (1 - core))
    ydev = (z * 2 + (1 - yl), fsdp)

    def zpos(dz):
        return (z + dz) % 4

    def zdev(dz):
        return (zpos(dz) * 2 + yl, fsdp)

    barrier = pltpu.get_barrier_semaphore()
    greet = [device(shifted(a, d)) for a in "xyz" for d in (1, -1)] + [zdev(2), partner]
    for who in greet:
        pl.semaphore_signal(barrier, inc=1, device_id=who, device_id_type=MESH)
    loads = [
        pltpu.make_async_copy(tokens, tok.at[0], loc.at[0]),
        pltpu.make_async_copy(deltas.at[0, :, yl], own0, loc.at[1]),
        pltpu.make_async_copy(deltas.at[1, z], own1, loc.at[2]),
        pltpu.make_async_copy(params.at[:, rep], pbuf, loc.at[3]),
        pltpu.make_async_copy(moment.at[:, rep], mbuf, loc.at[4]),
    ]
    for c in loads:
        c.start()
    pl.semaphore_wait(barrier, len(greet))

    sent = []

    def remote(src, dst, s, r, who):
        return pltpu.make_async_remote_copy(
            src_ref=src, dst_ref=dst, send_sem=s, recv_sem=r, device_id=who, device_id_type=MESH
        )

    def send(src, dst, s, r, who):
        c = remote(src, dst, s, r, who)
        c.start()
        sent.append(c)

    def landed(dst, s, r, who):
        remote(dst, dst, s, r, who).wait_recv()

    def lanes_at(half, first, count):
        return pl.ds(pl.multiple_of(half * HALF + first * LANES, LANES), count * LANES)

    def first_hop(s):
        out = []
        for h in range(2):
            cols = lanes_at(h, *SPANS[s])
            for dz in (2, 1, 3):
                out.append((deltas.at[1, zpos(dz), :, :, cols], rz1.at[dz - 1, :, :, cols], (s, h, dz), zdev(dz)))
            out.append((deltas.at[0, :, 1 - yl, :, cols], ry0.at[:, :, cols], (s, h, 0), ydev))
        return out

    def second_hop(s):
        out = []
        for h in range(2):
            cols = lanes_at(h, *SPANS[s])
            for dz in (2, 1, 3):
                out.append((pz0.at[dz - 1, :, cols], rz0.at[dz - 1, :, cols], (s, h, dz), zdev(dz)))
            out.append((pz1.at[:, cols], ry1.at[:, cols], (s, h, 0), ydev))
        return out

    def do_rs(s):
        for src, dst, i, who in first_hop(s):
            send(src, dst, a_s.at[i], a_r.at[i], who)
        if s == 0:
            send(tokens, tok.at[1], tk_s, tk_r, partner)

    def each_block(s, work):
        first, count = SPANS[s]

        def step(j, carry):
            work(j + first)
            return carry

        lax.fori_loop(0, count, step, 0)

    def do_rs2(s):
        if s == 0:
            for c in loads[1:]:
                c.wait()
        for _, dst, i, who in first_hop(s):
            landed(dst, a_s.at[i], a_r.at[i], who)

        def work(j):
            for h in range(2):
                cols = lanes_at(h, j, 1)
                for dz in (1, 2, 3):
                    v = own0[zpos(dz), :, cols].astype(f32) + ry0[zpos(dz), :, cols].astype(f32)
                    pz0[dz - 1, :, cols] = v.astype(bf16)
                v = own1[1 - yl, :, cols].astype(f32)
                for k in range(3):
                    v = v + rz1[k, 1 - yl, :, cols].astype(f32)
                pz1[:, cols] = v.astype(bf16)

        each_block(s, work)
        for src, dst, i, who in second_hop(s):
            send(src, dst, b_s.at[i], b_r.at[i], who)

    def do_upd(s):
        for _, dst, i, who in second_hop(s):
            landed(dst, b_s.at[i], b_r.at[i], who)

        def work(j):
            for other in (True, False):
                cols = lanes_at((1 - core) if other else core, j, 1)
                for mat in range(2):
                    if mat == 0:
                        v = own0[z, :, cols].astype(f32) + ry0[z, :, cols].astype(f32)
                        for k in range(3):
                            v = v + rz0[k, :, cols].astype(f32)
                    else:
                        v = own1[yl, :, cols].astype(f32)
                        for k in range(3):
                            v = v + rz1[k, yl, :, cols].astype(f32)
                        v = v + ry1[:, cols].astype(f32)
                    g = v * (1.0 / 8)
                    gsum[mat, z, yl, :, cols] = g.astype(bf16)
                    new, _ = advance(pbuf[mat, :, cols], mbuf[mat, :, cols], g)
                    lanes = pl.ds(mat * LANES, LANES)
                    if other:
                        stage[j, :, lanes] = new.astype(bf16)
                    else:
                        wts[j, yh, x, core, z, yl, :, lanes] = new.astype(bf16)

        each_block(s, work)
        us = pl.ds(*SPANS[s])
        send(stage.at[us], wts.at[us, yh, x, core, z, yl], dd_s.at[s], dd_r.at[s], partner)

    def do_dd(s):
        landed(wts.at[pl.ds(*SPANS[s]), yh, x, 1 - core, z, yl], dd_s.at[s], dd_r.at[s], partner)

    def region(us, at, half=ALL):
        fx = ALL if at["x"] is None else at["x"]
        fz = ALL if at["z"] is None else at["z"]
        fh, fl = (ALL, ALL) if at["y"] is None else (at["y"] // 2, at["y"] % 2)
        return wts.at[us, fh, fx, half, fz, fl]

    def ring(phase, part, first, count):
        order = ORDERS[part]
        axis = order[phase]
        row = phase * UNITS + first
        to = [device(shifted(axis, d)) for d in (1, -1)]

        def block(step, half=ALL):
            if part == "g":
                width = 2 * HALF * 2 // PIECES
                cols = pl.ds((first // 2) * width, width)
                return gsum.at[first % 2, (z + step + 4) % 4, half, :, cols]
            at = {a: (None if a in order[:phase] else here[a]) for a in "xyz"}
            return region(pl.ds(first, count), {**at, axis: (here[axis] + step + 4) % 4}, half)

        def sems(i):
            return (ring_s.at[row, i], ring_r.at[row, i], to[i % 2])

        return block, sems

    def do_st(*what):
        block, sems = ring(*what)
        for d in range(2):
            send(block(0), block(0), *sems(d))

    def do_fw(*what):
        block, sems = ring(*what)
        for d in range(2):
            back = -1 if d == 0 else 1
            landed(block(back), *sems(d))
            send(block(back, d), block(back, d), *sems(2 + d))

    def do_fi(*what):
        block, sems = ring(*what)
        for d in range(2):
            landed(block(2, d), *sems(2 + d))

    def do_gy0():
        own = gsum.at[:, z, yl]
        send(own, own, gy_s, gy_r, ydev)

    def do_gy1():
        landed(gsum.at[:, z, 1 - yl], gy_s, gy_r, ydev)

    waited = []

    def do_norm(part):
        count = 1024 // NORMS
        if not waited:
            loads[0].wait()
            waited.append(0)
        if len(waited) == 1 and (part + 1) * count > 512:
            landed(tok.at[1], tk_s, tk_r, partner)
            waited.append(1)
        chunk = 32

        def step(i, carry):
            i = i + part * (count // chunk)
            rows = pl.ds(pl.multiple_of((i % 16) * chunk, chunk), chunk)
            v = tok[i // 16, rows, :].astype(f32)
            scale = lax.rsqrt(jnp.mean(v * v, axis=-1, keepdims=True) + EPS)
            normed[pl.ds(pl.multiple_of(i * chunk, chunk), chunk), :] = (v * scale * gain[...]).astype(bf16)
            return carry

        lax.fori_loop(0, count // chunk, step, 0)

    factor = 1.0 / math.sqrt(2048)

    def do_mm(u):
        def step(m, carry):
            rows = pl.ds(pl.multiple_of(m * 512, 512), 512)
            w = wts[u].reshape(2048, 2 * LANES)
            out = jnp.dot(normed[rows, :], w, preferred_element_type=f32)
            gate = out[:, :LANES] * factor
            up = out[:, LANES:] * factor
            hbuf[u, m] = ((gate / (1.0 + jnp.exp(-gate))) * up).astype(bf16)
            return carry

        lax.fori_loop(0, 2, step, 0)

    copies = []

    def hidden_cols(c, u):
        return hidden.at[:, lanes_at(c, u, 1)]

    def do_em(u):
        c = pltpu.make_async_copy(hbuf.at[u, 0], hidden_cols(core, u), h_l.at[u])
        c.start()
        copies.append(c)
        send(hbuf.at[u, 1], hidden_cols(core, u), h_s.at[u], h_r.at[u], partner)

    does = {
        "rs": do_rs, "rs2": do_rs2, "upd": do_upd, "dd": do_dd, "st": do_st, "fw": do_fw, "fi": do_fi,
        "gy0": do_gy0, "gy1": do_gy1, "norm": do_norm, "mm": do_mm, "em": do_em,
    }
    ends = [i for i, op in enumerate(PLAN) if op[0] == "fi" and op[2] == "g"]
    for i, op in enumerate(PLAN):
        does[op[0]](*op[1:])
        if i == ends[-1]:
            c = pltpu.make_async_copy(gsum, grads, loc.at[5])
            c.start()
            copies.append(c)

    for c in copies:
        c.wait()
    for u in range(UNITS):
        landed(hidden_cols(1 - core, u), h_s.at[u], h_r.at[u], partner)
    for c in sent:
        c.wait_send()


def body(tokens, norm_gain, outer_params, momentum, deltas):
    bf16, f32 = jnp.bfloat16, jnp.float32
    hbm = pl.BlockSpec(memory_space=pl.ANY)
    dma = pltpu.SemaphoreType.DMA
    vmem = pltpu.VMEM
    spans = len(SPANS)
    hidden, grads = pl.pallas_call(
        kernel,
        out_shape=(
            jax.ShapeDtypeStruct((512, 4096), bf16),
            jax.ShapeDtypeStruct((2, 4, 2, 16, 4096), bf16),
        ),
        in_specs=[hbm, pl.BlockSpec(memory_space=pltpu.VMEM), hbm, hbm, hbm],
        out_specs=(hbm, hbm),
        scratch_shapes=[
            vmem((UNITS, 2, 4, 2, 4, 2, 16, 2 * LANES), bf16),
            vmem((2, 512, 2048), bf16),
            vmem((1024, 2048), bf16),
            vmem((4, 16, 4096), bf16),
            vmem((2, 16, 4096), bf16),
            vmem((4, 16, 4096), bf16),
            vmem((3, 16, 4096), bf16),
            vmem((3, 2, 16, 4096), bf16),
            vmem((16, 4096), bf16),
            vmem((3, 16, 4096), bf16),
            vmem((16, 4096), bf16),
            vmem((2, 16, 4096), f32),
            vmem((2, 16, 4096), f32),
            vmem((2, 4, 2, 16, 4096), bf16),
            vmem((UNITS, 16, 2 * LANES), bf16),
            vmem((UNITS, 2, 512, LANES), bf16),
            dma((6,)),
            dma((spans, 2, 4)), dma((spans, 2, 4)),
            dma((spans, 2, 4)), dma((spans, 2, 4)),
            dma, dma,
            dma((spans,)), dma((spans,)),
            dma((3 * UNITS + PIECES, 4)), dma((3 * UNITS + PIECES, 4)),
            dma, dma,
            dma((UNITS,)), dma((UNITS,)), dma((UNITS,)),
        ],
        compiler_params=pltpu.CompilerParams(
            collective_id=0, has_side_effects=True, vmem_limit_bytes=62 * 1024 * 1024
        ),
        name="outer_round",
    )(
        tokens,
        norm_gain.reshape(1, 2048),
        outer_params.reshape(2, 8, 16, 4096),
        momentum.reshape(2, 8, 16, 4096),
        deltas.reshape(2, 4, 2, 16, 4096),
    )
    outer_grad = grads.reshape(2, 128, 4096).astype(f32)
    new_params, new_momentum = advance(outer_params, momentum, outer_grad)
    return (new_params, new_momentum, hidden)


def solution(mesh):
    in_specs = (
        P(("rep", "fsdp"), None),
        P(),
        P(None, "fsdp", None),
        P(None, "fsdp", None),
        P("rep", None, "fsdp", None),
    )
    out_specs = (P(None, "fsdp", None), P(None, "fsdp", None), P(("rep", "fsdp"), None))
    return jax.shard_map(body, mesh=mesh, in_specs=in_specs, out_specs=out_specs, check_vma=False)
```

```python
import math

import jax
import jax.numpy as jnp
from jax import lax
from jax.experimental import pallas as pl
from jax.experimental.pallas import tpu as pltpu
from jax.sharding import PartitionSpec as P

EPS = 1e-05
MU = 0.9
RATE = 0.7
MESH = pl.DeviceIdType.MESH
ALL = slice(None)
UNITS = 16
LANES = 128
HALF = 2048

ORDERS = {'x': ('y', 'z', 'x'), 'y': ('z', 'x', 'y'), 'z': ('x', 'y', 'z'), 'g': ('z', 'z', 'z', 'z')}
SPANS = ((0, 5), (5, 5), (10, 2), (12, 4))
PIECES = 2
NORMS = 4
SKEWED = (1, 5, 6, 13)
PLAN = (
    ('rs', 0), ('rs', 1), ('rs2', 0), ('rs', 2),
    ('norm', 0), ('norm', 1), ('norm', 2), ('rs2', 1),
    ('rs', 3), ('norm', 3), ('upd', 0), ('st', 0, 'z', 3, 2),
    ('st', 0, 'x', 0, 1), ('st', 0, 'y', 1, 2), ('rs2', 2), ('dd', 0),
    ('upd', 1), ('st', 0, 'z', 8, 2), ('st', 0, 'x', 5, 2), ('st', 0, 'y', 7, 1),
    ('fi', 0, 'z', 3, 2), ('st', 1, 'z', 3, 1), ('st', 1, 'z', 4, 1), ('fi', 0, 'x', 0, 1),
    ('st', 1, 'x', 0, 1), ('dd', 1), ('rs2', 3), ('fi', 0, 'y', 1, 2),
    ('st', 1, 'y', 1, 1), ('st', 1, 'y', 2, 1), ('upd', 2), ('st', 0, 'x', 10, 1),
    ('st', 0, 'y', 11, 1), ('fi', 0, 'y', 7, 1), ('st', 1, 'y', 7, 1), ('fi', 0, 'x', 5, 2),
    ('st', 1, 'x', 5, 1), ('st', 1, 'x', 6, 1), ('fi', 0, 'z', 8, 2), ('st', 1, 'z', 8, 1),
    ('st', 1, 'z', 9, 1), ('fw', 1, 'z', 3, 1), ('fw', 1, 'x', 0, 1), ('dd', 2),
    ('fw', 1, 'z', 4, 1), ('fw', 1, 'y', 1, 1), ('upd', 3), ('st', 0, 'x', 12, 2),
    ('gy0',), ('st', 0, 'y', 14, 2), ('fi', 0, 'y', 11, 1), ('st', 1, 'y', 11, 1),
    ('fi', 0, 'x', 10, 1), ('st', 1, 'x', 10, 1), ('fw', 1, 'y', 2, 1), ('fw', 1, 'x', 5, 1),
    ('fw', 1, 'z', 8, 1), ('fw', 1, 'y', 7, 1), ('fw', 1, 'x', 6, 1), ('fi', 1, 'y', 1, 1),
    ('st', 2, 'y', 1, 1), ('dd', 3), ('fi', 1, 'x', 0, 1), ('st', 2, 'x', 0, 1),
    ('fi', 1, 'z', 3, 1), ('st', 2, 'z', 3, 1), ('fi', 1, 'z', 4, 1), ('fw', 1, 'z', 9, 1),
    ('fi', 0, 'y', 14, 2), ('fw', 1, 'y', 11, 1), ('fi', 1, 'y', 2, 1), ('st', 2, 'y', 2, 1),
    ('st', 1, 'y', 14, 1), ('fi', 0, 'x', 12, 2), ('fi', 1, 'y', 7, 1), ('fi', 1, 'x', 5, 1),
    ('fw', 1, 'x', 10, 1), ('fi', 1, 'x', 6, 1), ('st', 1, 'y', 15, 1), ('st', 1, 'x', 12, 1),
    ('gy1',), ('st', 2, 'x', 5, 1), ('st', 2, 'y', 7, 1), ('st', 1, 'x', 13, 1),
    ('st', 2, 'z', 4, 1), ('fi', 1, 'z', 8, 1), ('fi', 1, 'y', 11, 1), ('fi', 1, 'x', 10, 1),
    ('fw', 1, 'y', 14, 1), ('fw', 2, 'x', 0, 1), ('st', 2, 'y', 11, 1), ('fw', 1, 'x', 12, 1),
    ('fw', 1, 'x', 13, 1), ('fw', 2, 'z', 3, 1), ('fi', 1, 'z', 9, 1), ('fw', 1, 'y', 15, 1),
    ('fw', 2, 'x', 5, 1), ('st', 2, 'z', 8, 1), ('fi', 1, 'y', 14, 1), ('st', 2, 'x', 6, 1),
    ('fw', 2, 'y', 1, 1), ('fi', 1, 'x', 12, 1), ('fi', 1, 'x', 13, 1), ('fi', 2, 'x', 0, 1),
    ('mm', 0), ('em', 0), ('fw', 2, 'z', 4, 1), ('fi', 1, 'y', 15, 1),
    ('fi', 2, 'z', 3, 1), ('mm', 3), ('em', 3), ('st', 2, 'x', 10, 1),
    ('fw', 2, 'y', 2, 1), ('fi', 2, 'x', 5, 1), ('mm', 5), ('em', 5),
    ('st', 2, 'z', 9, 1), ('fw', 2, 'y', 7, 1), ('fw', 2, 'x', 6, 1), ('st', 2, 'y', 14, 1),
    ('fi', 2, 'y', 1, 1), ('fw', 2, 'z', 8, 1), ('fi', 2, 'z', 4, 1), ('mm', 1),
    ('em', 1), ('st', 2, 'x', 12, 1), ('mm', 4), ('em', 4),
    ('st', 3, 'g', 0, 1), ('fi', 2, 'y', 2, 1), ('mm', 2), ('em', 2),
    ('fw', 2, 'y', 11, 1), ('fi', 2, 'y', 7, 1), ('mm', 7), ('em', 7),
    ('fw', 2, 'x', 10, 1), ('st', 2, 'y', 15, 1), ('fi', 2, 'x', 6, 1), ('fw', 2, 'z', 9, 1),
    ('mm', 6), ('em', 6), ('st', 2, 'x', 13, 1), ('fi', 2, 'z', 8, 1),
    ('mm', 8), ('em', 8), ('st', 3, 'g', 1, 1), ('fw', 2, 'y', 14, 1),
    ('fi', 2, 'y', 11, 1), ('mm', 11), ('em', 11), ('fw', 2, 'x', 12, 1),
    ('fi', 2, 'x', 10, 1), ('fw', 3, 'g', 0, 1), ('mm', 10), ('em', 10),
    ('fi', 2, 'z', 9, 1), ('mm', 9), ('em', 9), ('fw', 2, 'y', 15, 1),
    ('fw', 2, 'x', 13, 1), ('fw', 3, 'g', 1, 1), ('fi', 2, 'y', 14, 1), ('mm', 14),
    ('em', 14), ('fi', 2, 'x', 12, 1), ('mm', 12), ('em', 12),
    ('fi', 3, 'g', 0, 1), ('fi', 2, 'y', 15, 1), ('mm', 15), ('em', 15),
    ('fi', 2, 'x', 13, 1), ('mm', 13), ('em', 13), ('fi', 3, 'g', 1, 1),
)


def advance(params, moment, outer_grad):
    moment_next = MU * moment + outer_grad
    params_next = params - RATE * (outer_grad + MU * moment_next)
    return (params_next, moment_next)


def kernel(
    tokens, gain_in, params, moment, deltas, hidden, grads,
    gain, wts, tok, normed, own0, own1, ry0, rz0, rz1, ry1, pz0, pz1, pbuf, mbuf, gsum, stage, hbuf,
    loc, a_s, a_r, b_s, b_r, tk_s, tk_r, dd_s, dd_r, line_s, line_r, ring_s, ring_r, gy_s, gy_r, h_l, h_s, h_r,
):
    bf16, f32 = jnp.bfloat16, jnp.float32
    rep = lax.axis_index("rep")
    fsdp = lax.axis_index("fsdp")
    z, yl = rep // 2, rep % 2
    yh, x, core = fsdp // 8, (fsdp // 2) % 4, fsdp % 2
    here = {"x": x, "y": yh * 2 + yl, "z": z}

    def device(at, c=core):
        return (at["z"] * 2 + at["y"] % 2, (at["y"] // 2) * 8 + at["x"] * 2 + c)

    def shifted(axis, step):
        return {**here, axis: (here[axis] + step + 4) % 4}

    partner = (rep, yh * 8 + x * 2 + (1 - core))
    ydev = (z * 2 + (1 - yl), fsdp)

    def zpos(dz):
        return (z + dz) % 4

    def zdev(dz):
        return (zpos(dz) * 2 + yl, fsdp)

    barrier = pltpu.get_barrier_semaphore()
    greet = [device(shifted(a, d), c) for a in "xyz" for d in (1, 2, 3) for c in (core, 1 - core)] + [partner]
    for who in greet:
        pl.semaphore_signal(barrier, inc=1, device_id=who, device_id_type=MESH)
    loads = [
        pltpu.make_async_copy(tokens, tok.at[0], loc.at[0]),
        pltpu.make_async_copy(deltas.at[0, :, yl], own0, loc.at[1]),
        pltpu.make_async_copy(deltas.at[1, z], own1, loc.at[2]),
        pltpu.make_async_copy(params.at[:, rep], pbuf, loc.at[3]),
        pltpu.make_async_copy(moment.at[:, rep], mbuf, loc.at[4]),
        pltpu.make_async_copy(gain_in, gain, loc.at[6]),
    ]
    for c in loads:
        c.start()
    pl.semaphore_wait(barrier, len(greet))

    sent = []

    def remote(src, dst, s, r, who):
        return pltpu.make_async_remote_copy(
            src_ref=src, dst_ref=dst, send_sem=s, recv_sem=r, device_id=who, device_id_type=MESH
        )

    def send(src, dst, s, r, who):
        c = remote(src, dst, s, r, who)
        c.start()
        sent.append(c)

    def landed(dst, s, r, who):
        remote(dst, dst, s, r, who).wait_recv()

    def lanes_at(half, first, count):
        return pl.ds(pl.multiple_of(half * HALF + first * LANES, LANES), count * LANES)

    def first_hop(s):
        out = []
        for h in range(2):
            cols = lanes_at(h, *SPANS[s])
            for dz in (2, 1, 3):
                out.append((deltas.at[1, zpos(dz), :, :, cols], rz1.at[dz - 1, :, :, cols], (s, h, dz), zdev(dz)))
            out.append((deltas.at[0, :, 1 - yl, :, cols], ry0.at[:, :, cols], (s, h, 0), ydev))
        return out

    def second_hop(s):
        out = []
        for h in range(2):
            cols = lanes_at(h, *SPANS[s])
            for dz in (2, 1, 3):
                out.append((pz0.at[dz - 1, :, cols], rz0.at[dz - 1, :, cols], (s, h, dz), zdev(dz)))
            out.append((pz1.at[:, cols], ry1.at[:, cols], (s, h, 0), ydev))
        return out

    def do_rs(s):
        for src, dst, i, who in first_hop(s):
            send(src, dst, a_s.at[i], a_r.at[i], who)
        if s == 0:
            send(tokens, tok.at[1], tk_s, tk_r, partner)

    def each_block(s, work):
        first, count = SPANS[s]

        def step(j, carry):
            work(j + first)
            return carry

        lax.fori_loop(0, count, step, 0)

    def do_rs2(s):
        if s == 0:
            for c in loads[1:-1]:
                c.wait()
        for _, dst, i, who in first_hop(s):
            landed(dst, a_s.at[i], a_r.at[i], who)

        def work(j):
            for h in range(2):
                cols = lanes_at(h, j, 1)
                for dz in (1, 2, 3):
                    v = own0[zpos(dz), :, cols].astype(f32) + ry0[zpos(dz), :, cols].astype(f32)
                    pz0[dz - 1, :, cols] = v.astype(bf16)
                v = own1[1 - yl, :, cols].astype(f32)
                for k in range(3):
                    v = v + rz1[k, 1 - yl, :, cols].astype(f32)
                pz1[:, cols] = v.astype(bf16)

        each_block(s, work)
        for src, dst, i, who in second_hop(s):
            send(src, dst, b_s.at[i], b_r.at[i], who)

    def do_upd(s):
        for _, dst, i, who in second_hop(s):
            landed(dst, b_s.at[i], b_r.at[i], who)

        def work(j):
            for other in (True, False):
                cols = lanes_at((1 - core) if other else core, j, 1)
                for mat in range(2):
                    if mat == 0:
                        v = own0[z, :, cols].astype(f32) + ry0[z, :, cols].astype(f32)
                        for k in range(3):
                            v = v + rz0[k, :, cols].astype(f32)
                    else:
                        v = own1[yl, :, cols].astype(f32)
                        for k in range(3):
                            v = v + rz1[k, yl, :, cols].astype(f32)
                        v = v + ry1[:, cols].astype(f32)
                    g = v * (1.0 / 8)
                    gsum[mat, z, yl, :, cols] = g.astype(bf16)
                    new, _ = advance(pbuf[mat, :, cols], mbuf[mat, :, cols], g)
                    lanes = pl.ds(mat * LANES, LANES)
                    if other:
                        stage[j, :, lanes] = new.astype(bf16)
                    else:
                        wts[j, yh, x, core, z, yl, :, lanes] = new.astype(bf16)

        each_block(s, work)
        us = pl.ds(*SPANS[s])
        send(stage.at[us], wts.at[us, yh, x, core, z, yl], dd_s.at[s], dd_r.at[s], partner)

    def do_dd(s):
        landed(wts.at[pl.ds(*SPANS[s]), yh, x, 1 - core, z, yl], dd_s.at[s], dd_r.at[s], partner)

    def region(us, at, half=ALL):
        fx = ALL if at["x"] is None else at["x"]
        fz = ALL if at["z"] is None else at["z"]
        fh, fl = (ALL, ALL) if at["y"] is None else (at["y"] // 2, at["y"] % 2)
        return wts.at[us, fh, fx, half, fz, fl]

    def lines(part, first, count):
        axis = ORDERS[part][0]
        us = pl.ds(first, count)
        for i, step in enumerate((2, 1, 3)):
            for k in range(2):
                row = core if k == 0 else 1 - core
                at = shifted(axis, -step)
                lands = wts.at[us, at["y"] // 2, at["x"], row, at["z"], at["y"] % 2]
                mine = wts.at[us, yh, x, core, z, yl]
                yield (mine if k == 0 else stage.at[us]), mine, lands, (
                    line_s.at[first, 2 * i + k], line_r.at[first, 2 * i + k], device(shifted(axis, step), row))

    def ring(phase, part, first, count):
        order = ORDERS[part]
        axis = order[phase]
        row = (phase - 1) * UNITS + first
        toward = 1 - 2 * yl if axis == "y" else 1
        steps = (toward, -toward)
        to = [device(shifted(axis, d)) for d in steps]

        def block(step, half=ALL):
            if part == "g":
                width = 2 * HALF * 2 // PIECES
                cols = pl.ds((first // 2) * width, width)
                return gsum.at[first % 2, (z + step + 4) % 4, half, :, cols]
            at = {a: (None if a in order[:phase] else here[a]) for a in "xyz"}
            return region(pl.ds(first, count), {**at, axis: (here[axis] + step + 4) % 4}, half)

        def sems(i):
            return (ring_s.at[row, i], ring_r.at[row, i], to[i % 2])

        came = steps if axis == "y" else (-steps[0], -steps[1])
        onward = (1, 0) if axis == "y" else (0, 1)
        if axis == "y" and first in SKEWED:
            carried = (None, ALL)
        else:
            carried = (0, 1)
        return block, sems, came, onward, carried

    def do_st(phase, part, first, count):
        if phase == 0:
            for src, dst, _, where in lines(part, first, count):
                send(src, dst, *where)
            return
        block, sems, _, _, _ = ring(phase, part, first, count)
        for d in range(2):
            send(block(0), block(0), *sems(d))

    def do_fw(*what):
        block, sems, came, onward, carried = ring(*what)
        for d in range(2):
            landed(block(came[d]), *sems(d))
            half = carried[onward[d]]
            if half is not None:
                part = block(came[d], half)
                send(part, part, *sems(2 + onward[d]))

    def do_fi(phase, part, first, count):
        if phase == 0:
            for _, _, lands, where in lines(part, first, count):
                landed(lands, *where)
            return
        block, sems, _, _, carried = ring(phase, part, first, count)
        for d in range(2):
            if carried[d] is not None:
                landed(block(2, carried[d]), *sems(2 + d))

    def do_gy0():
        own = gsum.at[:, z, yl]
        send(own, own, gy_s, gy_r, ydev)

    def do_gy1():
        landed(gsum.at[:, z, 1 - yl], gy_s, gy_r, ydev)

    waited = []

    def do_norm(part):
        count = 1024 // NORMS
        if not waited:
            loads[0].wait()
            loads[-1].wait()
            waited.append(0)
        if len(waited) == 1 and (part + 1) * count > 512:
            landed(tok.at[1], tk_s, tk_r, partner)
            waited.append(1)
        chunk = 32

        def step(i, carry):
            i = i + part * (count // chunk)
            rows = pl.ds(pl.multiple_of((i % 16) * chunk, chunk), chunk)
            v = tok[i // 16, rows, :].astype(f32)
            scale = lax.rsqrt(jnp.mean(v * v, axis=-1, keepdims=True) + EPS)
            normed[pl.ds(pl.multiple_of(i * chunk, chunk), chunk), :] = (v * scale * gain[...]).astype(bf16)
            return carry

        lax.fori_loop(0, count // chunk, step, 0)

    factor = 1.0 / math.sqrt(2048)

    def do_mm(u):
        def step(m, carry):
            rows = pl.ds(pl.multiple_of(m * 512, 512), 512)
            w = wts[u].reshape(2048, 2 * LANES)
            out = jnp.dot(normed[rows, :], w, preferred_element_type=f32)
            gate = out[:, :LANES] * factor
            up = out[:, LANES:] * factor
            hbuf[u, m] = ((gate / (1.0 + jnp.exp(-gate))) * up).astype(bf16)
            return carry

        lax.fori_loop(0, 2, step, 0)

    copies = []

    def hidden_cols(c, u):
        return hidden.at[:, lanes_at(c, u, 1)]

    def do_em(u):
        c = pltpu.make_async_copy(hbuf.at[u, 0], hidden_cols(core, u), h_l.at[u])
        c.start()
        copies.append(c)
        send(hbuf.at[u, 1], hidden_cols(core, u), h_s.at[u], h_r.at[u], partner)

    does = {
        "rs": do_rs, "rs2": do_rs2, "upd": do_upd, "dd": do_dd, "st": do_st, "fw": do_fw, "fi": do_fi,
        "gy0": do_gy0, "gy1": do_gy1, "norm": do_norm, "mm": do_mm, "em": do_em,
    }
    ends = [i for i, op in enumerate(PLAN) if op[0] == "fi" and op[2] == "g"]
    for i, op in enumerate(PLAN):
        does[op[0]](*op[1:])
        if i == ends[-1]:
            c = pltpu.make_async_copy(gsum, grads, loc.at[5])
            c.start()
            copies.append(c)

    for c in copies:
        c.wait()
    for u in range(UNITS):
        landed(hidden_cols(1 - core, u), h_s.at[u], h_r.at[u], partner)
    for c in sent:
        c.wait_send()


def held(a):
    return pltpu.with_memory_space_constraint(a, pltpu.HBM)


def body(tokens, norm_gain, outer_params, momentum, deltas):
    bf16, f32 = jnp.bfloat16, jnp.float32
    hbm = pl.BlockSpec(memory_space=pl.ANY)
    dma = pltpu.SemaphoreType.DMA
    vmem = pltpu.VMEM
    spans = len(SPANS)
    hidden, grads = pl.pallas_call(
        kernel,
        out_shape=(
            jax.ShapeDtypeStruct((512, 4096), bf16),
            jax.ShapeDtypeStruct((2, 4, 2, 16, 4096), bf16),
        ),
        in_specs=[hbm] * 5,
        out_specs=(hbm, hbm),
        scratch_shapes=[
            vmem((1, 2048), f32),
            vmem((UNITS, 2, 4, 2, 4, 2, 16, 2 * LANES), bf16),
            vmem((2, 512, 2048), bf16),
            vmem((1024, 2048), bf16),
            vmem((4, 16, 4096), bf16),
            vmem((2, 16, 4096), bf16),
            vmem((4, 16, 4096), bf16),
            vmem((3, 16, 4096), bf16),
            vmem((3, 2, 16, 4096), bf16),
            vmem((16, 4096), bf16),
            vmem((3, 16, 4096), bf16),
            vmem((16, 4096), bf16),
            vmem((2, 16, 4096), f32),
            vmem((2, 16, 4096), f32),
            vmem((2, 4, 2, 16, 4096), bf16),
            vmem((UNITS, 16, 2 * LANES), bf16),
            vmem((UNITS, 2, 512, LANES), bf16),
            dma((7,)),
            dma((spans, 2, 4)), dma((spans, 2, 4)),
            dma((spans, 2, 4)), dma((spans, 2, 4)),
            dma, dma,
            dma((spans,)), dma((spans,)),
            dma((UNITS, 6)), dma((UNITS, 6)),
            dma((2 * UNITS + PIECES, 4)), dma((2 * UNITS + PIECES, 4)),
            dma, dma,
            dma((UNITS,)), dma((UNITS,)), dma((UNITS,)),
        ],
        compiler_params=pltpu.CompilerParams(
            collective_id=0, has_side_effects=True, vmem_limit_bytes=44 * 1024 * 1024
        ),
        name="outer_round",
    )(
        held(tokens),
        held(norm_gain.reshape(1, 2048)),
        held(outer_params.reshape(2, 8, 16, 4096)),
        held(momentum.reshape(2, 8, 16, 4096)),
        held(deltas.reshape(2, 4, 2, 16, 4096)),
    )
    outer_grad = grads.reshape(2, 128, 4096).astype(f32)
    new_params, new_momentum = advance(outer_params, momentum, outer_grad)
    return (new_params, new_momentum, hidden)


def solution(mesh):
    in_specs = (
        P(("rep", "fsdp"), None),
        P(),
        P(None, "fsdp", None),
        P(None, "fsdp", None),
        P("rep", None, "fsdp", None),
    )
    out_specs = (P(None, "fsdp", None), P(None, "fsdp", None), P(("rep", "fsdp"), None))
    return jax.shard_map(body, mesh=mesh, in_specs=in_specs, out_specs=out_specs, check_vma=False)
```

```python
import math

import jax
import jax.numpy as jnp
from jax import lax
from jax.experimental import pallas as pl
from jax.experimental.pallas import tpu as pltpu
from jax.sharding import PartitionSpec as P

EPS = 1e-05
MU = 0.9
RATE = 0.7
MESH = pl.DeviceIdType.MESH
ALL = slice(None)
UNITS = 16
LANES = 128
HALF = 2048

ORDERS = {'x': ('y', 'z', 'x'), 'y': ('z', 'x', 'y'), 'z': ('x', 'y', 'z'), 'g': ('z', 'z', 'z', 'z')}
SPANS = ((0, 5), (5, 5), (10, 2), (12, 4))
PIECES = 2
NORMS = 4
SKEWED = (1, 5, 6, 13)
PLAN = (
    ('rs', 0), ('rs', 1), ('rs2', 0), ('rs', 2),
    ('norm', 0), ('norm', 1), ('norm', 2), ('rs2', 1),
    ('rs', 3), ('norm', 3), ('upd', 0), ('st', 0, 'z', 3, 2),
    ('st', 0, 'x', 0, 1), ('st', 0, 'y', 1, 2), ('rs2', 2), ('dd', 0),
    ('upd', 1), ('st', 0, 'z', 8, 2), ('st', 0, 'x', 5, 2), ('st', 0, 'y', 7, 1),
    ('fi', 0, 'z', 3, 2), ('st', 1, 'z', 3, 1), ('st', 1, 'z', 4, 1), ('fi', 0, 'x', 0, 1),
    ('st', 1, 'x', 0, 1), ('dd', 1), ('rs2', 3), ('fi', 0, 'y', 1, 2),
    ('st', 1, 'y', 1, 1), ('st', 1, 'y', 2, 1), ('upd', 2), ('st', 0, 'x', 10, 1),
    ('st', 0, 'y', 11, 1), ('fi', 0, 'y', 7, 1), ('st', 1, 'y', 7, 1), ('fi', 0, 'x', 5, 2),
    ('st', 1, 'x', 5, 1), ('st', 1, 'x', 6, 1), ('fi', 0, 'z', 8, 2), ('st', 1, 'z', 8, 1),
    ('st', 1, 'z', 9, 1), ('fw', 1, 'z', 3, 1), ('fw', 1, 'x', 0, 1), ('dd', 2),
    ('fw', 1, 'z', 4, 1), ('fw', 1, 'y', 1, 1), ('upd', 3), ('st', 0, 'x', 12, 2),
    ('gy0',), ('st', 0, 'y', 14, 2), ('fi', 0, 'y', 11, 1), ('st', 1, 'y', 11, 1),
    ('fi', 0, 'x', 10, 1), ('st', 1, 'x', 10, 1), ('fw', 1, 'y', 2, 1), ('fw', 1, 'x', 5, 1),
    ('fw', 1, 'z', 8, 1), ('fw', 1, 'y', 7, 1), ('fw', 1, 'x', 6, 1), ('fi', 1, 'y', 1, 1),
    ('st', 2, 'y', 1, 1), ('dd', 3), ('fi', 1, 'x', 0, 1), ('st', 2, 'x', 0, 1),
    ('fi', 1, 'z', 3, 1), ('st', 2, 'z', 3, 1), ('fi', 1, 'z', 4, 1), ('fw', 1, 'z', 9, 1),
    ('fi', 0, 'y', 14, 2), ('fw', 1, 'y', 11, 1), ('fi', 1, 'y', 2, 1), ('st', 2, 'y', 2, 1),
    ('st', 1, 'y', 14, 1), ('fi', 0, 'x', 12, 2), ('fi', 1, 'y', 7, 1), ('fi', 1, 'x', 5, 1),
    ('fw', 1, 'x', 10, 1), ('fi', 1, 'x', 6, 1), ('st', 1, 'y', 15, 1), ('st', 1, 'x', 12, 1),
    ('gy1',), ('st', 2, 'x', 5, 1), ('st', 2, 'y', 7, 1), ('st', 1, 'x', 13, 1),
    ('st', 2, 'z', 4, 1), ('fi', 1, 'z', 8, 1), ('fi', 1, 'y', 11, 1), ('fi', 1, 'x', 10, 1),
    ('fw', 1, 'y', 14, 1), ('fw', 2, 'x', 0, 1), ('st', 2, 'y', 11, 1), ('fw', 1, 'x', 12, 1),
    ('fw', 1, 'x', 13, 1), ('fw', 2, 'z', 3, 1), ('fi', 1, 'z', 9, 1), ('fw', 1, 'y', 15, 1),
    ('fw', 2, 'x', 5, 1), ('st', 2, 'z', 8, 1), ('fi', 1, 'y', 14, 1), ('st', 2, 'x', 6, 1),
    ('fw', 2, 'y', 1, 1), ('fi', 1, 'x', 12, 1), ('fi', 1, 'x', 13, 1), ('fi', 2, 'x', 0, 1),
    ('mm', 0), ('em', 0), ('fw', 2, 'z', 4, 1), ('fi', 1, 'y', 15, 1),
    ('fi', 2, 'z', 3, 1), ('mm', 3), ('em', 3), ('st', 2, 'x', 10, 1),
    ('fw', 2, 'y', 2, 1), ('fi', 2, 'x', 5, 1), ('mm', 5), ('em', 5),
    ('st', 2, 'z', 9, 1), ('fw', 2, 'y', 7, 1), ('fw', 2, 'x', 6, 1), ('st', 2, 'y', 14, 1),
    ('fi', 2, 'y', 1, 1), ('fw', 2, 'z', 8, 1), ('fi', 2, 'z', 4, 1), ('mm', 1),
    ('em', 1), ('st', 2, 'x', 12, 1), ('mm', 4), ('em', 4),
    ('st', 3, 'g', 0, 1), ('fi', 2, 'y', 2, 1), ('mm', 2), ('em', 2),
    ('fw', 2, 'y', 11, 1), ('fi', 2, 'y', 7, 1), ('mm', 7), ('em', 7),
    ('fw', 2, 'x', 10, 1), ('st', 2, 'y', 15, 1), ('fi', 2, 'x', 6, 1), ('fw', 2, 'z', 9, 1),
    ('mm', 6), ('em', 6), ('st', 2, 'x', 13, 1), ('fi', 2, 'z', 8, 1),
    ('mm', 8), ('em', 8), ('st', 3, 'g', 1, 1), ('fw', 2, 'y', 14, 1),
    ('fi', 2, 'y', 11, 1), ('mm', 11), ('em', 11), ('fw', 2, 'x', 12, 1),
    ('fi', 2, 'x', 10, 1), ('fw', 3, 'g', 0, 1), ('mm', 10), ('em', 10),
    ('fi', 2, 'z', 9, 1), ('mm', 9), ('em', 9), ('fw', 2, 'y', 15, 1),
    ('fw', 2, 'x', 13, 1), ('fw', 3, 'g', 1, 1), ('fi', 2, 'y', 14, 1), ('mm', 14),
    ('em', 14), ('fi', 2, 'x', 12, 1), ('mm', 12), ('em', 12),
    ('fi', 3, 'g', 0, 1), ('fi', 2, 'y', 15, 1), ('mm', 15), ('em', 15),
    ('fi', 2, 'x', 13, 1), ('mm', 13), ('em', 13), ('fi', 3, 'g', 1, 1),
)


def advance(params, moment, outer_grad):
    moment_next = MU * moment + outer_grad
    params_next = params - RATE * (outer_grad + MU * moment_next)
    return (params_next, moment_next)


def kernel(
    tokens, gain_in, params, moment, deltas, hidden, grads,
    gain, wts, tok, normed, own0, own1, ry0, rz0, rz1, ry1, pz0, pz1, pbuf, mbuf, gsum, stage, hbuf,
    loc, a_s, a_r, b_s, b_r, tk_s, tk_r, dd_s, dd_r, line_s, line_r, ring_s, ring_r, gy_s, gy_r, h_l, h_s, h_r,
):
    bf16, f32 = jnp.bfloat16, jnp.float32
    rep = lax.axis_index("rep")
    fsdp = lax.axis_index("fsdp")
    z, yl = rep // 2, rep % 2
    yh, x, core = fsdp // 8, (fsdp // 2) % 4, fsdp % 2
    here = {"x": x, "y": yh * 2 + yl, "z": z}

    def device(at, c=core):
        return (at["z"] * 2 + at["y"] % 2, (at["y"] // 2) * 8 + at["x"] * 2 + c)

    def shifted(axis, step):
        return {**here, axis: (here[axis] + step + 4) % 4}

    partner = (rep, yh * 8 + x * 2 + (1 - core))
    ydev = (z * 2 + (1 - yl), fsdp)

    def zpos(dz):
        return (z + dz) % 4

    def zdev(dz):
        return (zpos(dz) * 2 + yl, fsdp)

    barrier = pltpu.get_barrier_semaphore()
    greet = [device(shifted(a, d), c) for a in "xyz" for d in (1, 2, 3) for c in (core, 1 - core)] + [partner]
    for who in greet:
        pl.semaphore_signal(barrier, inc=1, device_id=who, device_id_type=MESH)
    loads = [
        pltpu.make_async_copy(tokens, tok.at[0], loc.at[0]),
        pltpu.make_async_copy(deltas.at[0, :, yl], own0, loc.at[1]),
        pltpu.make_async_copy(deltas.at[1, z], own1, loc.at[2]),
        pltpu.make_async_copy(params.at[:, rep], pbuf, loc.at[3]),
        pltpu.make_async_copy(moment.at[:, rep], mbuf, loc.at[4]),
        pltpu.make_async_copy(gain_in, gain, loc.at[6]),
    ]
    for c in loads:
        c.start()
    pl.semaphore_wait(barrier, len(greet))

    sent = []

    def remote(src, dst, s, r, who):
        return pltpu.make_async_remote_copy(
            src_ref=src, dst_ref=dst, send_sem=s, recv_sem=r, device_id=who, device_id_type=MESH
        )

    def send(src, dst, s, r, who):
        c = remote(src, dst, s, r, who)
        c.start()
        sent.append(c)

    def landed(dst, s, r, who):
        remote(dst, dst, s, r, who).wait_recv()

    def lanes_at(half, first, count):
        return pl.ds(pl.multiple_of(half * HALF + first * LANES, LANES), count * LANES)

    def first_hop(s):
        out = []
        for h in range(2):
            cols = lanes_at(h, *SPANS[s])
            for dz in (2, 1, 3):
                out.append((deltas.at[1, zpos(dz), :, :, cols], rz1.at[dz - 1, :, :, cols], (s, h, dz), zdev(dz)))
            out.append((deltas.at[0, :, 1 - yl, :, cols], ry0.at[:, :, cols], (s, h, 0), ydev))
        return out

    def second_hop(s):
        out = []
        for h in range(2):
            cols = lanes_at(h, *SPANS[s])
            for dz in (2, 1, 3):
                out.append((pz0.at[dz - 1, :, cols], rz0.at[dz - 1, :, cols], (s, h, dz), zdev(dz)))
            out.append((pz1.at[:, cols], ry1.at[:, cols], (s, h, 0), ydev))
        return out

    def do_rs(s):
        for src, dst, i, who in first_hop(s):
            send(src, dst, a_s.at[i], a_r.at[i], who)
        if s == 0:
            send(tokens, tok.at[1], tk_s, tk_r, partner)

    def each_block(s, work):
        first, count = SPANS[s]

        def step(j, carry):
            work(j + first)
            return carry

        lax.fori_loop(0, count, step, 0)

    def do_rs2(s):
        if s == 0:
            for c in loads[1:-1]:
                c.wait()
        for _, dst, i, who in first_hop(s):
            landed(dst, a_s.at[i], a_r.at[i], who)

        def work(j):
            for h in range(2):
                cols = lanes_at(h, j, 1)
                for dz in (1, 2, 3):
                    v = own0[zpos(dz), :, cols].astype(f32) + ry0[zpos(dz), :, cols].astype(f32)
                    pz0[dz - 1, :, cols] = v.astype(bf16)
                v = own1[1 - yl, :, cols].astype(f32)
                for k in range(3):
                    v = v + rz1[k, 1 - yl, :, cols].astype(f32)
                pz1[:, cols] = v.astype(bf16)

        each_block(s, work)
        for src, dst, i, who in second_hop(s):
            send(src, dst, b_s.at[i], b_r.at[i], who)

    def do_upd(s):
        for _, dst, i, who in second_hop(s):
            landed(dst, b_s.at[i], b_r.at[i], who)

        def work(j):
            for other in (True, False):
                cols = lanes_at((1 - core) if other else core, j, 1)
                for mat in range(2):
                    if mat == 0:
                        v = own0[z, :, cols].astype(f32) + ry0[z, :, cols].astype(f32)
                        for k in range(3):
                            v = v + rz0[k, :, cols].astype(f32)
                    else:
                        v = own1[yl, :, cols].astype(f32)
                        for k in range(3):
                            v = v + rz1[k, yl, :, cols].astype(f32)
                        v = v + ry1[:, cols].astype(f32)
                    g = v * (1.0 / 8)
                    gsum[mat, z, yl, :, cols] = g.astype(bf16)
                    new, _ = advance(pbuf[mat, :, cols], mbuf[mat, :, cols], g)
                    lanes = pl.ds(mat * LANES, LANES)
                    if other:
                        stage[j, :, lanes] = new.astype(bf16)
                    else:
                        wts[j, yh, x, core, z, yl, :, lanes] = new.astype(bf16)

        each_block(s, work)
        us = pl.ds(*SPANS[s])
        send(stage.at[us], wts.at[us, yh, x, core, z, yl], dd_s.at[s], dd_r.at[s], partner)

    def do_dd(s):
        landed(wts.at[pl.ds(*SPANS[s]), yh, x, 1 - core, z, yl], dd_s.at[s], dd_r.at[s], partner)

    def region(us, at, half=ALL):
        fx = ALL if at["x"] is None else at["x"]
        fz = ALL if at["z"] is None else at["z"]
        fh, fl = (ALL, ALL) if at["y"] is None else (at["y"] // 2, at["y"] % 2)
        return wts.at[us, fh, fx, half, fz, fl]

    def lines(part, first, count):
        axis = ORDERS[part][0]
        us = pl.ds(first, count)
        for i, step in enumerate((2, 1, 3)):
            for k in range(2):
                row = core if k == 0 else 1 - core
                at = shifted(axis, -step)
                lands = wts.at[us, at["y"] // 2, at["x"], row, at["z"], at["y"] % 2]
                mine = wts.at[us, yh, x, core, z, yl]
                yield (mine if k == 0 else stage.at[us]), mine, lands, (
                    line_s.at[first, 2 * i + k], line_r.at[first, 2 * i + k], device(shifted(axis, step), row))

    def ring(phase, part, first, count):
        order = ORDERS[part]
        axis = order[phase]
        row = (phase - 1) * UNITS + first
        toward = 1 - 2 * yl if axis == "y" else 1
        steps = (toward, -toward)
        to = [device(shifted(axis, d)) for d in steps]

        def block(step, half=ALL):
            if part == "g":
                width = 2 * HALF * 2 // PIECES
                cols = pl.ds((first // 2) * width, width)
                return gsum.at[first % 2, (z + step + 4) % 4, half, :, cols]
            at = {a: (None if a in order[:phase] else here[a]) for a in "xyz"}
            return region(pl.ds(first, count), {**at, axis: (here[axis] + step + 4) % 4}, half)

        def sems(i):
            return (ring_s.at[row, i], ring_r.at[row, i], to[i % 2])

        came = steps if axis == "y" else (-steps[0], -steps[1])
        onward = (1, 0) if axis == "y" else (0, 1)
        if axis == "y" and first in SKEWED:
            carried = (None, ALL)
        else:
            carried = (0, 1)
        return block, sems, came, onward, carried

    def do_st(phase, part, first, count):
        if phase == 0:
            for src, dst, _, where in lines(part, first, count):
                send(src, dst, *where)
            return
        block, sems, _, _, _ = ring(phase, part, first, count)
        for d in range(2):
            send(block(0), block(0), *sems(d))

    def do_fw(*what):
        block, sems, came, onward, carried = ring(*what)
        for d in range(2):
            landed(block(came[d]), *sems(d))
            half = carried[onward[d]]
            if half is not None:
                part = block(came[d], half)
                send(part, part, *sems(2 + onward[d]))

    def do_fi(phase, part, first, count):
        if phase == 0:
            for _, _, lands, where in lines(part, first, count):
                landed(lands, *where)
            return
        block, sems, _, _, carried = ring(phase, part, first, count)
        for d in range(2):
            if carried[d] is not None:
                landed(block(2, carried[d]), *sems(2 + d))

    def do_gy0():
        own = gsum.at[:, z, yl]
        send(own, own, gy_s, gy_r, ydev)

    def do_gy1():
        landed(gsum.at[:, z, 1 - yl], gy_s, gy_r, ydev)

    waited = []

    def do_norm(part):
        count = 1024 // NORMS
        if not waited:
            loads[0].wait()
            loads[-1].wait()
            waited.append(0)
        if len(waited) == 1 and (part + 1) * count > 512:
            landed(tok.at[1], tk_s, tk_r, partner)
            waited.append(1)
        chunk = 32

        def step(i, carry):
            i = i + part * (count // chunk)
            rows = pl.ds(pl.multiple_of((i % 16) * chunk, chunk), chunk)
            v = tok[i // 16, rows, :].astype(f32)
            scale = lax.rsqrt(jnp.mean(v * v, axis=-1, keepdims=True) + EPS)
            normed[pl.ds(pl.multiple_of(i * chunk, chunk), chunk), :] = (v * scale * gain[...]).astype(bf16)
            return carry

        lax.fori_loop(0, count // chunk, step, 0)

    factor = 1.0 / math.sqrt(2048)

    def do_mm(u):
        def step(m, carry):
            rows = pl.ds(pl.multiple_of(m * 512, 512), 512)
            w = wts[u].reshape(2048, 2 * LANES)
            out = jnp.dot(normed[rows, :], w, preferred_element_type=f32)
            gate = out[:, :LANES] * factor
            up = out[:, LANES:] * factor
            hbuf[u, m] = ((gate / (1.0 + jnp.exp(-gate))) * up).astype(bf16)
            return carry

        lax.fori_loop(0, 2, step, 0)

    copies = []

    def hidden_cols(c, u):
        return hidden.at[:, lanes_at(c, u, 1)]

    def do_em(u):
        c = pltpu.make_async_copy(hbuf.at[u, 0], hidden_cols(core, u), h_l.at[u])
        c.start()
        copies.append(c)
        send(hbuf.at[u, 1], hidden_cols(core, u), h_s.at[u], h_r.at[u], partner)

    does = {
        "rs": do_rs, "rs2": do_rs2, "upd": do_upd, "dd": do_dd, "st": do_st, "fw": do_fw, "fi": do_fi,
        "gy0": do_gy0, "gy1": do_gy1, "norm": do_norm, "mm": do_mm, "em": do_em,
    }
    ends = [i for i, op in enumerate(PLAN) if op[0] == "fi" and op[2] == "g"]
    for i, op in enumerate(PLAN):
        does[op[0]](*op[1:])
        if i == ends[-1]:
            c = pltpu.make_async_copy(gsum, grads, loc.at[5])
            c.start()
            copies.append(c)

    for c in copies:
        c.wait()
    for u in range(UNITS):
        landed(hidden_cols(1 - core, u), h_s.at[u], h_r.at[u], partner)
    for c in sent:
        c.wait_send()


def finish(params, moment, grads, rows, params_out, moment_out, rows_out, pbuf, mbuf, sems):
    copies = [pltpu.make_async_copy(rows, rows_out, sems.at[0, 0])]
    copies[0].start()
    for mat in range(2):
        for i in range(8):
            at = pl.ds(i * 16, 16)
            g = grads[mat, at, :].astype(jnp.float32)
            new, nxt = advance(params[mat, at, :], moment[mat, at, :], g)
            pbuf[mat, at, :] = new
            mbuf[mat, at, :] = nxt
            for k, (src, dst) in enumerate(((pbuf, params_out), (mbuf, moment_out))):
                copies.append(pltpu.make_async_copy(src.at[mat, at], dst.at[mat, at], sems.at[1 + k, mat * 8 + i]))
                copies[-1].start()
    for c in copies:
        c.wait()


def held(a):
    return pltpu.with_memory_space_constraint(a, pltpu.HBM)


def body(tokens, norm_gain, outer_params, momentum, deltas):
    bf16, f32 = jnp.bfloat16, jnp.float32
    hbm = pl.BlockSpec(memory_space=pl.ANY)
    dma = pltpu.SemaphoreType.DMA
    vmem = pltpu.VMEM
    spans = len(SPANS)
    hidden, grads = pl.pallas_call(
        kernel,
        out_shape=(
            jax.ShapeDtypeStruct((512, 4096), bf16),
            jax.ShapeDtypeStruct((2, 4, 2, 16, 4096), bf16),
        ),
        in_specs=[hbm] * 5,
        out_specs=(hbm, hbm),
        scratch_shapes=[
            vmem((1, 2048), f32),
            vmem((UNITS, 2, 4, 2, 4, 2, 16, 2 * LANES), bf16),
            vmem((2, 512, 2048), bf16),
            vmem((1024, 2048), bf16),
            vmem((4, 16, 4096), bf16),
            vmem((2, 16, 4096), bf16),
            vmem((4, 16, 4096), bf16),
            vmem((3, 16, 4096), bf16),
            vmem((3, 2, 16, 4096), bf16),
            vmem((16, 4096), bf16),
            vmem((3, 16, 4096), bf16),
            vmem((16, 4096), bf16),
            vmem((2, 16, 4096), f32),
            vmem((2, 16, 4096), f32),
            vmem((2, 4, 2, 16, 4096), bf16),
            vmem((UNITS, 16, 2 * LANES), bf16),
            vmem((UNITS, 2, 512, LANES), bf16),
            dma((7,)),
            dma((spans, 2, 4)), dma((spans, 2, 4)),
            dma((spans, 2, 4)), dma((spans, 2, 4)),
            dma, dma,
            dma((spans,)), dma((spans,)),
            dma((UNITS, 6)), dma((UNITS, 6)),
            dma((2 * UNITS + PIECES, 4)), dma((2 * UNITS + PIECES, 4)),
            dma, dma,
            dma((UNITS,)), dma((UNITS,)), dma((UNITS,)),
        ],
        compiler_params=pltpu.CompilerParams(
            collective_id=0, has_side_effects=True, vmem_limit_bytes=44 * 1024 * 1024
        ),
        name="outer_round",
    )(
        held(tokens),
        held(norm_gain.reshape(1, 2048)),
        held(outer_params.reshape(2, 8, 16, 4096)),
        held(momentum.reshape(2, 8, 16, 4096)),
        held(deltas.reshape(2, 4, 2, 16, 4096)),
    )
    here = pl.BlockSpec(memory_space=pltpu.VMEM)
    state = jax.ShapeDtypeStruct((2, 128, 4096), f32)
    return pl.pallas_call(
        finish,
        out_shape=(state, state, jax.ShapeDtypeStruct((512, 4096), bf16)),
        in_specs=[here] * 4,
        out_specs=(hbm, hbm, hbm),
        scratch_shapes=[vmem((2, 128, 4096), f32), vmem((2, 128, 4096), f32), dma((3, 16))],
        compiler_params=pltpu.CompilerParams(vmem_limit_bytes=28 * 1024 * 1024),
        name="finish",
    )(outer_params, momentum, grads.reshape(2, 128, 4096), hidden)


def solution(mesh):
    in_specs = (
        P(("rep", "fsdp"), None),
        P(),
        P(None, "fsdp", None),
        P(None, "fsdp", None),
        P("rep", None, "fsdp", None),
    )
    out_specs = (P(None, "fsdp", None), P(None, "fsdp", None), P(("rep", "fsdp"), None))
    return jax.shard_map(body, mesh=mesh, in_specs=in_specs, out_specs=out_specs, check_vma=False)
```

```python
import math

import jax
import jax.numpy as jnp
from jax import lax
from jax.experimental import pallas as pl
from jax.experimental.pallas import tpu as pltpu
from jax.sharding import PartitionSpec as P

EPS = 1e-05
MU = 0.9
RATE = 0.7
MESH = pl.DeviceIdType.MESH
ALL = slice(None)
UNITS = 16
LANES = 128
HALF = 2048

ORDERS = {'x': ('y', 'z', 'x'), 'y': ('z', 'x', 'y'), 'z': ('x', 'y', 'z'), 'g': ('z', 'z', 'z', 'z')}
SPANS = ((0, 3), (3, 4), (7, 3), (10, 3), (13, 3))
PIECES = 2
NORMS = 2
SKEWED = (2, 7, 8, 10, 11, 13)
PLAN = (
    ('rs', 0), ('rs', 1), ('rs2', 0), ('rs', 2),
    ('norm', 0), ('rs2', 1), ('rs', 3), ('norm', 1),
    ('upd', 0), ('st', 0, 'z', 2, 1), ('st', 0, 'x', 0, 1), ('st', 0, 'y', 1, 1),
    ('rs2', 2), ('rs', 4), ('dd', 0), ('upd', 1),
    ('st', 0, 'z', 5, 2), ('st', 0, 'x', 3, 1), ('st', 0, 'y', 4, 1), ('fi', 0, 'z', 2, 1),
    ('st', 1, 'z', 2, 1), ('fi', 0, 'x', 0, 1), ('st', 1, 'x', 0, 1), ('rs2', 3),
    ('fi', 0, 'y', 1, 1), ('st', 1, 'y', 1, 1), ('dd', 1), ('upd', 2),
    ('st', 0, 'z', 9, 1), ('st', 0, 'x', 7, 1), ('st', 0, 'y', 8, 1), ('fi', 0, 'z', 5, 2),
    ('st', 1, 'z', 5, 1), ('st', 1, 'z', 6, 1), ('fi', 0, 'x', 3, 1), ('st', 1, 'x', 3, 1),
    ('rs2', 4), ('fi', 0, 'y', 4, 1), ('st', 1, 'y', 4, 1), ('dd', 2),
    ('fw', 1, 'y', 1, 1), ('fw', 1, 'z', 2, 1), ('fw', 1, 'x', 0, 1), ('fi', 0, 'x', 7, 1),
    ('st', 1, 'x', 7, 1), ('fi', 0, 'z', 9, 1), ('st', 1, 'z', 9, 1), ('upd', 3),
    ('st', 0, 'x', 10, 2), ('st', 0, 'y', 12, 1), ('fi', 0, 'y', 8, 1), ('st', 1, 'y', 8, 1),
    ('fw', 1, 'z', 5, 1), ('fw', 1, 'x', 3, 1), ('fw', 1, 'y', 4, 1), ('fw', 1, 'z', 6, 1),
    ('fi', 1, 'y', 1, 1), ('st', 2, 'y', 1, 1), ('dd', 3), ('fi', 1, 'x', 0, 1),
    ('st', 2, 'x', 0, 1), ('fi', 1, 'z', 2, 1), ('st', 2, 'z', 2, 1), ('upd', 4),
    ('fw', 1, 'y', 8, 1), ('fi', 1, 'y', 4, 1), ('st', 0, 'y', 14, 2), ('fi', 1, 'x', 3, 1),
    ('st', 2, 'x', 3, 1), ('st', 0, 'x', 13, 1), ('fi', 0, 'y', 12, 1), ('dd', 4),
    ('fi', 1, 'z', 5, 1), ('fw', 1, 'z', 9, 1), ('fw', 1, 'x', 7, 1), ('fi', 0, 'x', 10, 2),
    ('st', 2, 'y', 4, 1), ('st', 1, 'x', 10, 1), ('fi', 1, 'z', 6, 1), ('st', 1, 'y', 12, 1),
    ('st', 1, 'x', 11, 1), ('st', 2, 'z', 5, 1), ('fi', 1, 'y', 8, 1), ('fw', 2, 'x', 0, 1),
    ('fw', 2, 'y', 1, 1), ('fi', 1, 'x', 7, 1), ('fi', 0, 'y', 14, 2), ('fi', 1, 'z', 9, 1),
    ('fi', 0, 'x', 13, 1), ('st', 1, 'y', 14, 1), ('st', 1, 'y', 15, 1), ('st', 2, 'y', 8, 1),
    ('fw', 1, 'x', 10, 1), ('fw', 1, 'x', 11, 1), ('st', 1, 'x', 13, 1), ('fw', 1, 'y', 12, 1),
    ('fw', 2, 'x', 3, 1), ('fw', 2, 'z', 2, 1), ('fi', 2, 'x', 0, 1), ('st', 2, 'x', 7, 1),
    ('fw', 2, 'y', 4, 1), ('st', 2, 'z', 6, 1), ('mm', 0), ('em', 0),
    ('gy0',), ('fi', 1, 'x', 10, 1), ('fi', 1, 'x', 11, 1), ('fi', 2, 'y', 1, 1),
    ('fi', 1, 'y', 12, 1), ('st', 2, 'y', 12, 1), ('mm', 1), ('em', 1),
    ('fw', 1, 'x', 13, 1), ('fi', 2, 'z', 2, 1), ('fw', 1, 'y', 14, 1), ('fw', 1, 'y', 15, 1),
    ('fw', 2, 'z', 5, 1), ('fi', 2, 'x', 3, 1), ('st', 2, 'x', 10, 1), ('mm', 2),
    ('em', 2), ('mm', 3), ('em', 3), ('fw', 2, 'y', 8, 1),
    ('st', 2, 'z', 9, 1), ('fi', 2, 'y', 4, 1), ('mm', 4), ('em', 4),
    ('fi', 1, 'x', 13, 1), ('fw', 2, 'x', 7, 1), ('fi', 1, 'y', 14, 1), ('fi', 1, 'y', 15, 1),
    ('st', 2, 'y', 14, 1), ('gy1',), ('fw', 2, 'z', 6, 1), ('fi', 2, 'z', 5, 1),
    ('st', 2, 'x', 11, 1), ('mm', 5), ('em', 5), ('st', 2, 'y', 15, 1),
    ('st', 3, 'g', 0, 1), ('fi', 2, 'y', 8, 1), ('fw', 2, 'x', 10, 1), ('mm', 8),
    ('em', 8), ('fi', 2, 'x', 7, 1), ('fw', 2, 'z', 9, 1), ('mm', 7),
    ('em', 7), ('st', 2, 'x', 13, 1), ('fi', 2, 'z', 6, 1), ('mm', 6),
    ('em', 6), ('fw', 2, 'y', 12, 1), ('st', 3, 'g', 1, 1), ('fw', 2, 'y', 14, 1),
    ('fw', 2, 'x', 11, 1), ('fi', 2, 'x', 10, 1), ('mm', 10), ('em', 10),
    ('fw', 3, 'g', 0, 1), ('fw', 2, 'y', 15, 1), ('fi', 2, 'z', 9, 1), ('mm', 9),
    ('em', 9), ('fi', 2, 'y', 12, 1), ('mm', 12), ('em', 12),
    ('fw', 2, 'x', 13, 1), ('fi', 2, 'y', 14, 1), ('fw', 3, 'g', 1, 1), ('mm', 14),
    ('em', 14), ('fi', 2, 'x', 11, 1), ('mm', 11), ('em', 11),
    ('fi', 2, 'y', 15, 1), ('fi', 3, 'g', 0, 1), ('mm', 15), ('em', 15),
    ('fi', 2, 'x', 13, 1), ('mm', 13), ('em', 13), ('fi', 3, 'g', 1, 1),
)


def advance(params, moment, outer_grad):
    moment_next = MU * moment + outer_grad
    params_next = params - RATE * (outer_grad + MU * moment_next)
    return (params_next, moment_next)


def kernel(
    tokens, gain_in, params, moment, deltas, hidden, grads,
    gain, wts, tok, normed, held, ry0, rz0, rz1, ry1, pz0, pz1, pbuf, mbuf, gsum, stage, hbuf,
    loc, a_s, a_r, b_s, b_r, tk_s, tk_r, dd_s, dd_r, line_s, line_r, ring_s, ring_r, gy_s, gy_r, h_l, h_s, h_r,
):
    bf16, f32 = jnp.bfloat16, jnp.float32
    rep = lax.axis_index("rep")
    fsdp = lax.axis_index("fsdp")
    z, yl = rep // 2, rep % 2
    yh, x, core = fsdp // 8, (fsdp // 2) % 4, fsdp % 2
    here = {"x": x, "y": yh * 2 + yl, "z": z}

    def device(at, c=core):
        return (at["z"] * 2 + at["y"] % 2, (at["y"] // 2) * 8 + at["x"] * 2 + c)

    def shifted(axis, step):
        return {**here, axis: (here[axis] + step + 4) % 4}

    partner = (rep, yh * 8 + x * 2 + (1 - core))
    ydev = (z * 2 + (1 - yl), fsdp)

    def zpos(dz):
        return (z + dz) % 4

    def zdev(dz):
        return (zpos(dz) * 2 + yl, fsdp)

    barrier = pltpu.get_barrier_semaphore()
    greet = [device(shifted(a, d), c) for a in "xyz" for d in (1, 2, 3) for c in (core, 1 - core)] + [partner]
    for who in greet:
        pl.semaphore_signal(barrier, inc=1, device_id=who, device_id_type=MESH)
    loads = [
        pltpu.make_async_copy(tokens, tok.at[0], loc.at[0]),
        pltpu.make_async_copy(params.at[:, rep], pbuf, loc.at[3]),
        pltpu.make_async_copy(moment.at[:, rep], mbuf, loc.at[4]),
        pltpu.make_async_copy(gain_in, gain, loc.at[6]),
    ]
    staged = pltpu.make_async_copy(deltas, held, loc.at[1])
    staged.start()
    pl.semaphore_wait(barrier, len(greet))
    for c in loads:
        c.start()
    staged.wait()

    sent = []

    def remote(src, dst, s, r, who):
        return pltpu.make_async_remote_copy(
            src_ref=src, dst_ref=dst, send_sem=s, recv_sem=r, device_id=who, device_id_type=MESH
        )

    def send(src, dst, s, r, who):
        c = remote(src, dst, s, r, who)
        c.start()
        sent.append(c)

    def landed(dst, s, r, who):
        remote(dst, dst, s, r, who).wait_recv()

    def lanes_at(half, first, count):
        return pl.ds(pl.multiple_of(half * HALF + first * LANES, LANES), count * LANES)

    def first_hop(s):
        out = []
        for h in range(2):
            cols = lanes_at(h, *SPANS[s])
            for dz in (2, 1, 3):
                out.append((held.at[1, zpos(dz), :, :, cols], rz1.at[dz - 1, :, :, cols], (s, h, dz), zdev(dz)))
            out.append((held.at[0, :, 1 - yl, :, cols], ry0.at[:, :, cols], (s, h, 0), ydev))
        return out

    def second_hop(s):
        out = []
        for h in range(2):
            cols = lanes_at(h, *SPANS[s])
            for dz in (2, 1, 3):
                out.append((pz0.at[dz - 1, :, cols], rz0.at[dz - 1, :, cols], (s, h, dz), zdev(dz)))
            out.append((pz1.at[:, cols], ry1.at[:, cols], (s, h, 0), ydev))
        return out

    def do_rs(s):
        for src, dst, i, who in first_hop(s):
            send(src, dst, a_s.at[i], a_r.at[i], who)
        if s == 0:
            send(tokens, tok.at[1], tk_s, tk_r, partner)

    def each_block(s, work):
        first, count = SPANS[s]

        def step(j, carry):
            work(j + first)
            return carry

        lax.fori_loop(0, count, step, 0)

    def do_rs2(s):
        if s == 0:
            for c in loads[1:-1]:
                c.wait()
        for _, dst, i, who in first_hop(s):
            landed(dst, a_s.at[i], a_r.at[i], who)

        def work(j):
            for h in range(2):
                cols = lanes_at(h, j, 1)
                for dz in (1, 2, 3):
                    v = held[0, zpos(dz), yl, :, cols].astype(f32) + ry0[zpos(dz), :, cols].astype(f32)
                    pz0[dz - 1, :, cols] = v.astype(bf16)
                v = held[1, z, 1 - yl, :, cols].astype(f32)
                for k in range(3):
                    v = v + rz1[k, 1 - yl, :, cols].astype(f32)
                pz1[:, cols] = v.astype(bf16)

        each_block(s, work)
        for src, dst, i, who in second_hop(s):
            send(src, dst, b_s.at[i], b_r.at[i], who)

    def do_upd(s):
        for _, dst, i, who in second_hop(s):
            landed(dst, b_s.at[i], b_r.at[i], who)

        def work(j):
            for other in (True, False):
                cols = lanes_at((1 - core) if other else core, j, 1)
                for mat in range(2):
                    if mat == 0:
                        v = held[0, z, yl, :, cols].astype(f32) + ry0[z, :, cols].astype(f32)
                        for k in range(3):
                            v = v + rz0[k, :, cols].astype(f32)
                    else:
                        v = held[1, z, yl, :, cols].astype(f32)
                        for k in range(3):
                            v = v + rz1[k, yl, :, cols].astype(f32)
                        v = v + ry1[:, cols].astype(f32)
                    g = v * (1.0 / 8)
                    gsum[mat, z, yl, :, cols] = g.astype(bf16)
                    new, _ = advance(pbuf[mat, :, cols], mbuf[mat, :, cols], g)
                    lanes = pl.ds(mat * LANES, LANES)
                    if other:
                        stage[j, :, lanes] = new.astype(bf16)
                    else:
                        wts[j, yh, x, core, z, yl, :, lanes] = new.astype(bf16)

        each_block(s, work)
        us = pl.ds(*SPANS[s])
        send(stage.at[us], wts.at[us, yh, x, core, z, yl], dd_s.at[s], dd_r.at[s], partner)

    def do_dd(s):
        landed(wts.at[pl.ds(*SPANS[s]), yh, x, 1 - core, z, yl], dd_s.at[s], dd_r.at[s], partner)

    def region(us, at, half=ALL):
        fx = ALL if at["x"] is None else at["x"]
        fz = ALL if at["z"] is None else at["z"]
        fh, fl = (ALL, ALL) if at["y"] is None else (at["y"] // 2, at["y"] % 2)
        return wts.at[us, fh, fx, half, fz, fl]

    def lines(part, first, count):
        axis = ORDERS[part][0]
        us = pl.ds(first, count)
        for i, step in enumerate((2, 1, 3)):
            for k in range(2):
                row = core if k == 0 else 1 - core
                at = shifted(axis, -step)
                lands = wts.at[us, at["y"] // 2, at["x"], row, at["z"], at["y"] % 2]
                mine = wts.at[us, yh, x, core, z, yl]
                yield (mine if k == 0 else stage.at[us]), mine, lands, (
                    line_s.at[first, 2 * i + k], line_r.at[first, 2 * i + k], device(shifted(axis, step), row))

    def ring(phase, part, first, count):
        order = ORDERS[part]
        axis = order[phase]
        row = (phase - 1) * UNITS + first
        toward = 1 - 2 * yl if axis == "y" else 1
        steps = (toward, -toward)
        to = [device(shifted(axis, d)) for d in steps]

        def block(step, half=ALL):
            if part == "g":
                width = 2 * HALF * 2 // PIECES
                cols = pl.ds((first // 2) * width, width)
                return gsum.at[first % 2, (z + step + 4) % 4, half, :, cols]
            at = {a: (None if a in order[:phase] else here[a]) for a in "xyz"}
            return region(pl.ds(first, count), {**at, axis: (here[axis] + step + 4) % 4}, half)

        def sems(i):
            return (ring_s.at[row, i], ring_r.at[row, i], to[i % 2])

        came = steps if axis == "y" else (-steps[0], -steps[1])
        onward = (1, 0) if axis == "y" else (0, 1)
        if axis == "y" and first in SKEWED:
            carried = (None, ALL)
        else:
            carried = (0, 1)
        return block, sems, came, onward, carried

    def do_st(phase, part, first, count):
        if phase == 0:
            for src, dst, _, where in lines(part, first, count):
                send(src, dst, *where)
            return
        block, sems, _, _, _ = ring(phase, part, first, count)
        for d in range(2):
            send(block(0), block(0), *sems(d))

    def do_fw(*what):
        block, sems, came, onward, carried = ring(*what)
        for d in range(2):
            landed(block(came[d]), *sems(d))
            half = carried[onward[d]]
            if half is not None:
                part = block(came[d], half)
                send(part, part, *sems(2 + onward[d]))

    def do_fi(phase, part, first, count):
        if phase == 0:
            for _, _, lands, where in lines(part, first, count):
                landed(lands, *where)
            return
        block, sems, _, _, carried = ring(phase, part, first, count)
        for d in range(2):
            if carried[d] is not None:
                landed(block(2, carried[d]), *sems(2 + d))

    def do_gy0():
        own = gsum.at[:, z, yl]
        send(own, own, gy_s, gy_r, ydev)

    def do_gy1():
        landed(gsum.at[:, z, 1 - yl], gy_s, gy_r, ydev)

    waited = []

    def do_norm(part):
        count = 1024 // NORMS
        if not waited:
            loads[0].wait()
            loads[-1].wait()
            waited.append(0)
        if len(waited) == 1 and (part + 1) * count > 512:
            landed(tok.at[1], tk_s, tk_r, partner)
            waited.append(1)
        chunk = 32

        def step(i, carry):
            i = i + part * (count // chunk)
            rows = pl.ds(pl.multiple_of((i % 16) * chunk, chunk), chunk)
            v = tok[i // 16, rows, :].astype(f32)
            scale = lax.rsqrt(jnp.mean(v * v, axis=-1, keepdims=True) + EPS)
            normed[pl.ds(pl.multiple_of(i * chunk, chunk), chunk), :] = (v * scale * gain[...]).astype(bf16)
            return carry

        lax.fori_loop(0, count // chunk, step, 0)

    factor = 1.0 / math.sqrt(2048)

    last = [op[1] for op in PLAN if op[0] == "mm"][-1]

    def do_mm(u):
        def step(m, carry):
            rows = pl.ds(pl.multiple_of(m * 512, 512), 512)
            w = wts[u].reshape(2048, 2 * LANES)
            out = jnp.dot(normed[rows, :], w, preferred_element_type=f32)
            gate = out[:, :LANES] * factor
            up = out[:, LANES:] * factor
            hbuf[u, m] = ((gate / (1.0 + jnp.exp(-gate))) * up).astype(bf16)
            return carry

        if u == last:
            step(1, 0)
            away(u)
            step(0, 0)
        else:
            lax.fori_loop(0, 2, step, 0)

    copies = []

    def away(u):
        send(hbuf.at[u, 1], hidden_cols(core, u), h_s.at[u], h_r.at[u], partner)

    def hidden_cols(c, u):
        return hidden.at[:, lanes_at(c, u, 1)]

    def do_em(u):
        c = pltpu.make_async_copy(hbuf.at[u, 0], hidden_cols(core, u), h_l.at[u])
        c.start()
        copies.append(c)
        if u != last:
            away(u)

    does = {
        "rs": do_rs, "rs2": do_rs2, "upd": do_upd, "dd": do_dd, "st": do_st, "fw": do_fw, "fi": do_fi,
        "gy0": do_gy0, "gy1": do_gy1, "norm": do_norm, "mm": do_mm, "em": do_em,
    }
    ends = [i for i, op in enumerate(PLAN) if op[0] == "fi" and op[2] == "g"]
    for i, op in enumerate(PLAN):
        does[op[0]](*op[1:])
        if i == ends[-1]:
            c = pltpu.make_async_copy(gsum, grads, loc.at[5])
            c.start()
            copies.append(c)

    for c in copies:
        c.wait()
    for u in range(UNITS):
        landed(hidden_cols(1 - core, u), h_s.at[u], h_r.at[u], partner)
    for c in sent:
        c.wait_send()


def finish(params, moment, grads, rows, params_out, moment_out, rows_out, pbuf, mbuf, sems):
    copies = [pltpu.make_async_copy(rows, rows_out, sems.at[0, 0])]
    copies[0].start()
    for mat in range(2):
        for i in range(8):
            at = pl.ds(i * 16, 16)
            g = grads[mat, at, :].astype(jnp.float32)
            new, nxt = advance(params[mat, at, :], moment[mat, at, :], g)
            pbuf[mat, at, :] = new
            mbuf[mat, at, :] = nxt
            for k, (src, dst) in enumerate(((pbuf, params_out), (mbuf, moment_out))):
                copies.append(pltpu.make_async_copy(src.at[mat, at], dst.at[mat, at], sems.at[1 + k, mat * 8 + i]))
                copies[-1].start()
    for c in copies:
        c.wait()


def in_hbm(a):
    return pltpu.with_memory_space_constraint(a, pltpu.HBM)


def body(tokens, norm_gain, outer_params, momentum, deltas):
    bf16, f32 = jnp.bfloat16, jnp.float32
    hbm = pl.BlockSpec(memory_space=pl.ANY)
    dma = pltpu.SemaphoreType.DMA
    vmem = pltpu.VMEM
    spans = len(SPANS)
    hidden, grads = pl.pallas_call(
        kernel,
        out_shape=(
            jax.ShapeDtypeStruct((512, 4096), bf16),
            jax.ShapeDtypeStruct((2, 4, 2, 16, 4096), bf16),
        ),
        in_specs=[hbm] * 5,
        out_specs=(hbm, hbm),
        scratch_shapes=[
            vmem((1, 2048), f32),
            vmem((UNITS, 2, 4, 2, 4, 2, 16, 2 * LANES), bf16),
            vmem((2, 512, 2048), bf16),
            vmem((1024, 2048), bf16),
            vmem((2, 4, 2, 16, 4096), bf16),
            vmem((4, 16, 4096), bf16),
            vmem((3, 16, 4096), bf16),
            vmem((3, 2, 16, 4096), bf16),
            vmem((16, 4096), bf16),
            vmem((3, 16, 4096), bf16),
            vmem((16, 4096), bf16),
            vmem((2, 16, 4096), f32),
            vmem((2, 16, 4096), f32),
            vmem((2, 4, 2, 16, 4096), bf16),
            vmem((UNITS, 16, 2 * LANES), bf16),
            vmem((UNITS, 2, 512, LANES), bf16),
            dma((7,)),
            dma((spans, 2, 4)), dma((spans, 2, 4)),
            dma((spans, 2, 4)), dma((spans, 2, 4)),
            dma, dma,
            dma((spans,)), dma((spans,)),
            dma((UNITS, 6)), dma((UNITS, 6)),
            dma((2 * UNITS + PIECES, 4)), dma((2 * UNITS + PIECES, 4)),
            dma, dma,
            dma((UNITS,)), dma((UNITS,)), dma((UNITS,)),
        ],
        compiler_params=pltpu.CompilerParams(
            collective_id=0, has_side_effects=True, vmem_limit_bytes=44 * 1024 * 1024
        ),
        name="outer_round",
    )(
        in_hbm(tokens),
        in_hbm(norm_gain.reshape(1, 2048)),
        in_hbm(outer_params.reshape(2, 8, 16, 4096)),
        in_hbm(momentum.reshape(2, 8, 16, 4096)),
        in_hbm(deltas.reshape(2, 4, 2, 16, 4096)),
    )
    here = pl.BlockSpec(memory_space=pltpu.VMEM)
    state = jax.ShapeDtypeStruct((2, 128, 4096), f32)
    return pl.pallas_call(
        finish,
        out_shape=(state, state, jax.ShapeDtypeStruct((512, 4096), bf16)),
        in_specs=[here] * 4,
        out_specs=(hbm, hbm, hbm),
        scratch_shapes=[vmem((2, 128, 4096), f32), vmem((2, 128, 4096), f32), dma((3, 16))],
        compiler_params=pltpu.CompilerParams(vmem_limit_bytes=28 * 1024 * 1024),
        name="finish",
    )(outer_params, momentum, grads.reshape(2, 128, 4096), hidden)


def solution(mesh):
    in_specs = (
        P(("rep", "fsdp"), None),
        P(),
        P(None, "fsdp", None),
        P(None, "fsdp", None),
        P("rep", None, "fsdp", None),
    )
    out_specs = (P(None, "fsdp", None), P(None, "fsdp", None), P(("rep", "fsdp"), None))
    return jax.shard_map(body, mesh=mesh, in_specs=in_specs, out_specs=out_specs, check_vma=False)
```

```python
import math

import jax
import jax.numpy as jnp
from jax import lax
from jax.experimental import pallas as pl
from jax.experimental.pallas import tpu as pltpu
from jax.sharding import PartitionSpec as P

EPS = 1e-05
MU = 0.9
RATE = 0.7
MESH = pl.DeviceIdType.MESH
ALL = slice(None)
UNITS = 16
LANES = 128
HALF = 2048

ORDERS = {'x': ('y', 'z', 'x'), 'y': ('z', 'x', 'y'), 'z': ('x', 'y', 'z'), 'g': ('z', 'z', 'z', 'z')}
SPANS = ((0, 4), (4, 5), (9, 4), (13, 3))
PIECES = 2
NORMS = 4
SKEWED = (0, 6, 8, 9)
PLAN = (
    ('rs', 0), ('rs', 1), ('rs2', 0), ('rs', 2),
    ('norm', 0), ('norm', 1), ('norm', 2), ('rs2', 1),
    ('rs', 3), ('norm', 3), ('upd', 0), ('st', 0, 'z', 2, 2),
    ('st', 0, 'x', 0, 1), ('dd', 0), ('st', 0, 'y', 1, 1), ('rs2', 2),
    ('upd', 1), ('st', 0, 'z', 8, 1), ('st', 0, 'x', 4, 2), ('st', 0, 'y', 6, 2),
    ('fi', 0, 'x', 0, 1), ('st', 1, 'x', 0, 1), ('fi', 0, 'z', 2, 2), ('st', 1, 'z', 2, 1),
    ('rs2', 3), ('st', 1, 'z', 3, 1), ('fi', 0, 'y', 1, 1), ('st', 1, 'y', 1, 1),
    ('dd', 1), ('upd', 2), ('st', 0, 'z', 12, 1), ('st', 0, 'x', 9, 2),
    ('st', 0, 'y', 11, 1), ('fi', 0, 'z', 8, 1), ('st', 1, 'z', 8, 1), ('fi', 0, 'y', 6, 2),
    ('st', 1, 'y', 6, 1), ('st', 1, 'y', 7, 1), ('fi', 0, 'x', 4, 2), ('st', 1, 'x', 4, 1),
    ('st', 1, 'x', 5, 1), ('fw', 1, 'z', 2, 1), ('dd', 2), ('fw', 1, 'y', 1, 1),
    ('fw', 1, 'z', 3, 1), ('fw', 1, 'x', 0, 1), ('upd', 3), ('st', 0, 'x', 13, 1),
    ('gy0',), ('st', 0, 'y', 14, 2), ('fi', 0, 'y', 11, 1), ('st', 1, 'y', 11, 1),
    ('fi', 0, 'z', 12, 1), ('st', 1, 'z', 12, 1), ('fw', 1, 'y', 6, 1), ('fw', 1, 'x', 4, 1),
    ('fi', 0, 'x', 9, 2), ('st', 1, 'x', 9, 1), ('dd', 3), ('fw', 1, 'z', 8, 1),
    ('fw', 1, 'y', 7, 1), ('st', 1, 'x', 10, 1), ('fi', 1, 'z', 2, 1), ('fi', 1, 'y', 1, 1),
    ('st', 2, 'y', 1, 1), ('fi', 1, 'z', 3, 1), ('fi', 1, 'x', 0, 1), ('st', 2, 'x', 0, 1),
    ('fw', 1, 'x', 5, 1), ('st', 2, 'z', 2, 1), ('fi', 0, 'x', 13, 1), ('fi', 1, 'y', 6, 1),
    ('fi', 1, 'x', 4, 1), ('fi', 0, 'y', 14, 2), ('fi', 1, 'y', 7, 1), ('fi', 1, 'z', 8, 1),
    ('fw', 1, 'y', 11, 1), ('st', 2, 'y', 6, 1), ('fi', 1, 'x', 5, 1), ('st', 1, 'y', 14, 1),
    ('gy1',), ('st', 1, 'y', 15, 1), ('fw', 1, 'x', 9, 1), ('fw', 1, 'x', 10, 1),
    ('fw', 2, 'x', 0, 1), ('st', 2, 'z', 3, 1), ('fi', 1, 'y', 11, 1), ('fw', 1, 'y', 14, 1),
    ('fw', 1, 'z', 12, 1), ('st', 2, 'y', 7, 1), ('fi', 1, 'x', 9, 1), ('st', 2, 'x', 4, 1),
    ('fi', 1, 'x', 10, 1), ('fi', 2, 'x', 0, 1), ('fw', 2, 'z', 2, 1), ('mm', 0),
    ('em', 0), ('fw', 2, 'y', 1, 1), ('fi', 1, 'y', 14, 1), ('fw', 1, 'y', 15, 1),
    ('st', 2, 'x', 5, 1), ('fw', 2, 'z', 3, 1), ('fi', 1, 'z', 12, 1), ('fw', 2, 'y', 6, 1),
    ('st', 2, 'z', 8, 1), ('fi', 2, 'z', 2, 1), ('mm', 2), ('em', 2),
    ('fi', 1, 'y', 15, 1), ('fi', 2, 'z', 3, 1), ('fw', 2, 'x', 4, 1), ('st', 2, 'y', 11, 1),
    ('mm', 3), ('em', 3), ('st', 1, 'x', 13, 1), ('fw', 2, 'x', 5, 1),
    ('st', 2, 'z', 12, 1), ('fi', 2, 'y', 1, 1), ('mm', 1), ('em', 1),
    ('st', 2, 'x', 9, 1), ('fw', 2, 'y', 7, 1), ('fi', 2, 'y', 6, 1), ('mm', 6),
    ('em', 6), ('fi', 2, 'x', 4, 1), ('mm', 4), ('em', 4),
    ('st', 2, 'y', 14, 1), ('fw', 2, 'z', 8, 1), ('fi', 2, 'x', 5, 1), ('mm', 5),
    ('em', 5), ('st', 2, 'x', 10, 1), ('fw', 1, 'x', 13, 1), ('fw', 2, 'z', 12, 1),
    ('fi', 2, 'y', 7, 1), ('mm', 7), ('em', 7), ('fw', 2, 'y', 11, 1),
    ('st', 3, 'g', 0, 1), ('fi', 2, 'z', 8, 1), ('mm', 8), ('em', 8),
    ('fw', 2, 'x', 9, 1), ('st', 2, 'y', 15, 1), ('fi', 1, 'x', 13, 1), ('st', 2, 'x', 13, 1),
    ('fi', 2, 'z', 12, 1), ('mm', 12), ('em', 12), ('st', 3, 'g', 1, 1),
    ('fi', 2, 'y', 11, 1), ('mm', 11), ('em', 11), ('fw', 2, 'y', 14, 1),
    ('fi', 2, 'x', 9, 1), ('mm', 9), ('em', 9), ('fw', 2, 'x', 10, 1),
    ('fw', 2, 'y', 15, 1), ('fw', 3, 'g', 0, 1), ('fw', 2, 'x', 13, 1), ('fi', 2, 'y', 14, 1),
    ('fw', 3, 'g', 1, 1), ('mm', 14), ('em', 14), ('fi', 2, 'x', 10, 1),
    ('mm', 10), ('em', 10), ('fi', 3, 'g', 0, 1), ('fi', 2, 'y', 15, 1),
    ('mm', 15), ('em', 15), ('fi', 2, 'x', 13, 1), ('mm', 13),
    ('em', 13), ('fi', 3, 'g', 1, 1),
)


def advance(params, moment, outer_grad):
    moment_next = MU * moment + outer_grad
    params_next = params - RATE * (outer_grad + MU * moment_next)
    return (params_next, moment_next)


def kernel(
    tokens, gain_in, params, moment, deltas, hidden, grads,
    gain, wts, tok, normed, held, ry0, rz0, rz1, ry1, pz0, pz1, pbuf, mbuf, gsum, stage, hbuf,
    loc, a_s, a_r, b_s, b_r, tk_s, tk_r, dd_s, dd_r, line_s, line_r, ring_s, ring_r, gy_s, gy_r, h_l, h_s, h_r,
):
    bf16, f32 = jnp.bfloat16, jnp.float32
    rep = lax.axis_index("rep")
    fsdp = lax.axis_index("fsdp")
    z, yl = rep // 2, rep % 2
    yh, x, core = fsdp // 8, (fsdp // 2) % 4, fsdp % 2
    here = {"x": x, "y": yh * 2 + yl, "z": z}

    def device(at, c=core):
        return (at["z"] * 2 + at["y"] % 2, (at["y"] // 2) * 8 + at["x"] * 2 + c)

    def shifted(axis, step):
        return {**here, axis: (here[axis] + step + 4) % 4}

    partner = (rep, yh * 8 + x * 2 + (1 - core))
    ydev = (z * 2 + (1 - yl), fsdp)

    def zpos(dz):
        return (z + dz) % 4

    def zdev(dz):
        return (zpos(dz) * 2 + yl, fsdp)

    barrier = pltpu.get_barrier_semaphore()
    greet = [device(shifted(a, d), c) for a in "xyz" for d in (1, 2, 3) for c in (core, 1 - core)] + [partner]
    for who in greet:
        pl.semaphore_signal(barrier, inc=1, device_id=who, device_id_type=MESH)
    loads = [
        pltpu.make_async_copy(tokens, tok.at[0], loc.at[0]),
        pltpu.make_async_copy(params.at[:, rep], pbuf, loc.at[3]),
        pltpu.make_async_copy(moment.at[:, rep], mbuf, loc.at[4]),
        pltpu.make_async_copy(gain_in, gain, loc.at[6]),
    ]
    staged = pltpu.make_async_copy(deltas, held, loc.at[1])
    staged.start()
    pl.semaphore_wait(barrier, len(greet))
    for c in loads:
        c.start()
    staged.wait()

    sent = []

    def remote(src, dst, s, r, who):
        return pltpu.make_async_remote_copy(
            src_ref=src, dst_ref=dst, send_sem=s, recv_sem=r, device_id=who, device_id_type=MESH
        )

    def send(src, dst, s, r, who):
        c = remote(src, dst, s, r, who)
        c.start()
        sent.append(c)

    def landed(dst, s, r, who):
        remote(dst, dst, s, r, who).wait_recv()

    def lanes_at(half, first, count):
        return pl.ds(pl.multiple_of(half * HALF + first * LANES, LANES), count * LANES)

    def first_hop(s):
        out = []
        for h in range(2):
            cols = lanes_at(h, *SPANS[s])
            for dz in (2, 1, 3):
                out.append((held.at[1, zpos(dz), :, :, cols], rz1.at[dz - 1, :, :, cols], (s, h, dz), zdev(dz)))
            out.append((held.at[0, :, 1 - yl, :, cols], ry0.at[:, :, cols], (s, h, 0), ydev))
        return out

    def second_hop(s):
        out = []
        for h in range(2):
            cols = lanes_at(h, *SPANS[s])
            for dz in (2, 1, 3):
                out.append((pz0.at[dz - 1, :, cols], rz0.at[dz - 1, :, cols], (s, h, dz), zdev(dz)))
            out.append((pz1.at[:, cols], ry1.at[:, cols], (s, h, 0), ydev))
        return out

    def do_rs(s):
        for src, dst, i, who in first_hop(s):
            send(src, dst, a_s.at[i], a_r.at[i], who)
        if s == 0:
            send(tokens, tok.at[1], tk_s, tk_r, partner)

    def each_block(s, work):
        first, count = SPANS[s]

        def step(j, carry):
            work(j + first)
            return carry

        lax.fori_loop(0, count, step, 0)

    def do_rs2(s):
        if s == 0:
            for c in loads[1:-1]:
                c.wait()
        for _, dst, i, who in first_hop(s):
            landed(dst, a_s.at[i], a_r.at[i], who)

        def work(j):
            for h in range(2):
                cols = lanes_at(h, j, 1)
                for dz in (1, 2, 3):
                    v = held[0, zpos(dz), yl, :, cols].astype(f32) + ry0[zpos(dz), :, cols].astype(f32)
                    pz0[dz - 1, :, cols] = v.astype(bf16)
                v = held[1, z, 1 - yl, :, cols].astype(f32)
                for k in range(3):
                    v = v + rz1[k, 1 - yl, :, cols].astype(f32)
                pz1[:, cols] = v.astype(bf16)

        each_block(s, work)
        for src, dst, i, who in second_hop(s):
            send(src, dst, b_s.at[i], b_r.at[i], who)

    def do_upd(s):
        for _, dst, i, who in second_hop(s):
            landed(dst, b_s.at[i], b_r.at[i], who)

        def work(j):
            for other in (True, False):
                cols = lanes_at((1 - core) if other else core, j, 1)
                for mat in range(2):
                    if mat == 0:
                        v = held[0, z, yl, :, cols].astype(f32) + ry0[z, :, cols].astype(f32)
                        for k in range(3):
                            v = v + rz0[k, :, cols].astype(f32)
                    else:
                        v = held[1, z, yl, :, cols].astype(f32)
                        for k in range(3):
                            v = v + rz1[k, yl, :, cols].astype(f32)
                        v = v + ry1[:, cols].astype(f32)
                    g = v * (1.0 / 8)
                    gsum[mat, z, yl, :, cols] = g.astype(bf16)
                    new, _ = advance(pbuf[mat, :, cols], mbuf[mat, :, cols], g)
                    lanes = pl.ds(mat * LANES, LANES)
                    if other:
                        stage[j, :, lanes] = new.astype(bf16)
                    else:
                        wts[j, yh, x, core, z, yl, :, lanes] = new.astype(bf16)

        each_block(s, work)
        us = pl.ds(*SPANS[s])
        send(stage.at[us], wts.at[us, yh, x, core, z, yl], dd_s.at[s], dd_r.at[s], partner)

    def do_dd(s):
        landed(wts.at[pl.ds(*SPANS[s]), yh, x, 1 - core, z, yl], dd_s.at[s], dd_r.at[s], partner)

    def region(us, at, half=ALL):
        fx = ALL if at["x"] is None else at["x"]
        fz = ALL if at["z"] is None else at["z"]
        fh, fl = (ALL, ALL) if at["y"] is None else (at["y"] // 2, at["y"] % 2)
        return wts.at[us, fh, fx, half, fz, fl]

    def lines(part, first, count):
        axis = ORDERS[part][0]
        us = pl.ds(first, count)
        for i, step in enumerate((2, 1, 3)):
            for k in range(2):
                row = core if k == 0 else 1 - core
                at = shifted(axis, -step)
                lands = wts.at[us, at["y"] // 2, at["x"], row, at["z"], at["y"] % 2]
                mine = wts.at[us, yh, x, core, z, yl]
                yield (mine if k == 0 else stage.at[us]), mine, lands, (
                    line_s.at[first, 2 * i + k], line_r.at[first, 2 * i + k], device(shifted(axis, step), row))

    def ring(phase, part, first, count):
        order = ORDERS[part]
        axis = order[phase]
        row = (phase - 1) * UNITS + first
        toward = 1 - 2 * yl if axis == "y" else 1
        steps = (toward, -toward)
        to = [device(shifted(axis, d)) for d in steps]

        def block(step, half=ALL):
            if part == "g":
                width = 2 * HALF * 2 // PIECES
                cols = pl.ds((first // 2) * width, width)
                return gsum.at[first % 2, (z + step + 4) % 4, half, :, cols]
            at = {a: (None if a in order[:phase] else here[a]) for a in "xyz"}
            return region(pl.ds(first, count), {**at, axis: (here[axis] + step + 4) % 4}, half)

        def sems(i):
            return (ring_s.at[row, i], ring_r.at[row, i], to[i % 2])

        came = steps if axis == "y" else (-steps[0], -steps[1])
        onward = (1, 0) if axis == "y" else (0, 1)
        if axis == "y" and first in SKEWED:
            carried = (None, ALL)
        else:
            carried = (0, 1)
        return block, sems, came, onward, carried

    def do_st(phase, part, first, count):
        if phase == 0:
            for src, dst, _, where in lines(part, first, count):
                send(src, dst, *where)
            return
        block, sems, _, _, _ = ring(phase, part, first, count)
        for d in range(2):
            send(block(0), block(0), *sems(d))

    def do_fw(*what):
        block, sems, came, onward, carried = ring(*what)
        for d in range(2):
            landed(block(came[d]), *sems(d))
            half = carried[onward[d]]
            if half is not None:
                part = block(came[d], half)
                send(part, part, *sems(2 + onward[d]))

    def do_fi(phase, part, first, count):
        if phase == 0:
            for _, _, lands, where in lines(part, first, count):
                landed(lands, *where)
            return
        block, sems, _, _, carried = ring(phase, part, first, count)
        for d in range(2):
            if carried[d] is not None:
                landed(block(2, carried[d]), *sems(2 + d))

    def do_gy0():
        own = gsum.at[:, z, yl]
        send(own, own, gy_s, gy_r, ydev)

    def do_gy1():
        landed(gsum.at[:, z, 1 - yl], gy_s, gy_r, ydev)

    waited = []

    def do_norm(part):
        count = 1024 // NORMS
        if not waited:
            loads[0].wait()
            loads[-1].wait()
            waited.append(0)
        if len(waited) == 1 and (part + 1) * count > 512:
            landed(tok.at[1], tk_s, tk_r, partner)
            waited.append(1)
        chunk = 32

        def step(i, carry):
            i = i + part * (count // chunk)
            rows = pl.ds(pl.multiple_of((i % 16) * chunk, chunk), chunk)
            v = tok[i // 16, rows, :].astype(f32)
            scale = lax.rsqrt(jnp.mean(v * v, axis=-1, keepdims=True) + EPS)
            normed[pl.ds(pl.multiple_of(i * chunk, chunk), chunk), :] = (v * scale * gain[...]).astype(bf16)
            return carry

        lax.fori_loop(0, count // chunk, step, 0)

    factor = 1.0 / math.sqrt(2048)

    def do_mm(u):
        def step(m, carry):
            rows = pl.ds(pl.multiple_of(m * 512, 512), 512)
            w = wts[u].reshape(2048, 2 * LANES)
            out = jnp.dot(normed[rows, :], w, preferred_element_type=f32)
            gate = out[:, :LANES] * factor
            up = out[:, LANES:] * factor
            hbuf[u, m] = ((gate / (1.0 + jnp.exp(-gate))) * up).astype(bf16)
            return carry

        lax.fori_loop(0, 2, step, 0)

    copies = []

    def away(u):
        send(hbuf.at[u, 1], hidden_cols(core, u), h_s.at[u], h_r.at[u], partner)

    def hidden_cols(c, u):
        return hidden.at[:, lanes_at(c, u, 1)]

    def do_em(u):
        c = pltpu.make_async_copy(hbuf.at[u, 0], hidden_cols(core, u), h_l.at[u])
        c.start()
        copies.append(c)
        away(u)

    does = {
        "rs": do_rs, "rs2": do_rs2, "upd": do_upd, "dd": do_dd, "st": do_st, "fw": do_fw, "fi": do_fi,
        "gy0": do_gy0, "gy1": do_gy1, "norm": do_norm, "mm": do_mm, "em": do_em,
    }
    ends = [i for i, op in enumerate(PLAN) if op[0] == "fi" and op[2] == "g"]
    for i, op in enumerate(PLAN):
        does[op[0]](*op[1:])
        if i == ends[-1]:
            c = pltpu.make_async_copy(gsum, grads, loc.at[5])
            c.start()
            copies.append(c)

    for c in copies:
        c.wait()
    for u in range(UNITS):
        landed(hidden_cols(1 - core, u), h_s.at[u], h_r.at[u], partner)
    for c in sent:
        c.wait_send()


def finish(params, moment, grads, rows, params_out, moment_out, rows_out, pbuf, mbuf, sems):
    copies = [pltpu.make_async_copy(rows, rows_out, sems.at[0, 0])]
    copies[0].start()
    for mat in range(2):
        for i in range(8):
            at = pl.ds(i * 16, 16)
            g = grads[mat, at, :].astype(jnp.float32)
            new, nxt = advance(params[mat, at, :], moment[mat, at, :], g)
            pbuf[mat, at, :] = new
            mbuf[mat, at, :] = nxt
            for k, (src, dst) in enumerate(((pbuf, params_out), (mbuf, moment_out))):
                copies.append(pltpu.make_async_copy(src.at[mat, at], dst.at[mat, at], sems.at[1 + k, mat * 8 + i]))
                copies[-1].start()
    for c in copies:
        c.wait()


def in_hbm(a):
    return pltpu.with_memory_space_constraint(a, pltpu.HBM)


def body(tokens, norm_gain, outer_params, momentum, deltas):
    bf16, f32 = jnp.bfloat16, jnp.float32
    hbm = pl.BlockSpec(memory_space=pl.ANY)
    dma = pltpu.SemaphoreType.DMA
    vmem = pltpu.VMEM
    spans = len(SPANS)
    hidden, grads = pl.pallas_call(
        kernel,
        out_shape=(
            jax.ShapeDtypeStruct((512, 4096), bf16),
            jax.ShapeDtypeStruct((2, 4, 2, 16, 4096), bf16),
        ),
        in_specs=[hbm] * 5,
        out_specs=(hbm, hbm),
        scratch_shapes=[
            vmem((1, 2048), f32),
            vmem((UNITS, 2, 4, 2, 4, 2, 16, 2 * LANES), bf16),
            vmem((2, 512, 2048), bf16),
            vmem((1024, 2048), bf16),
            vmem((2, 4, 2, 16, 4096), bf16),
            vmem((4, 16, 4096), bf16),
            vmem((3, 16, 4096), bf16),
            vmem((3, 2, 16, 4096), bf16),
            vmem((16, 4096), bf16),
            vmem((3, 16, 4096), bf16),
            vmem((16, 4096), bf16),
            vmem((2, 16, 4096), f32),
            vmem((2, 16, 4096), f32),
            vmem((2, 4, 2, 16, 4096), bf16),
            vmem((UNITS, 16, 2 * LANES), bf16),
            vmem((UNITS, 2, 512, LANES), bf16),
            dma((7,)),
            dma((spans, 2, 4)), dma((spans, 2, 4)),
            dma((spans, 2, 4)), dma((spans, 2, 4)),
            dma, dma,
            dma((spans,)), dma((spans,)),
            dma((UNITS, 6)), dma((UNITS, 6)),
            dma((2 * UNITS + PIECES, 4)), dma((2 * UNITS + PIECES, 4)),
            dma, dma,
            dma((UNITS,)), dma((UNITS,)), dma((UNITS,)),
        ],
        compiler_params=pltpu.CompilerParams(
            collective_id=0, has_side_effects=True, vmem_limit_bytes=44 * 1024 * 1024
        ),
        name="outer_round",
    )(
        in_hbm(tokens),
        in_hbm(norm_gain.reshape(1, 2048)),
        in_hbm(outer_params.reshape(2, 8, 16, 4096)),
        in_hbm(momentum.reshape(2, 8, 16, 4096)),
        in_hbm(deltas.reshape(2, 4, 2, 16, 4096)),
    )
    here = pl.BlockSpec(memory_space=pltpu.VMEM)
    state = jax.ShapeDtypeStruct((2, 128, 4096), f32)
    return pl.pallas_call(
        finish,
        out_shape=(state, state, jax.ShapeDtypeStruct((512, 4096), bf16)),
        in_specs=[here] * 4,
        out_specs=(hbm, hbm, hbm),
        scratch_shapes=[vmem((2, 128, 4096), f32), vmem((2, 128, 4096), f32), dma((3, 16))],
        compiler_params=pltpu.CompilerParams(vmem_limit_bytes=28 * 1024 * 1024),
        name="finish",
    )(outer_params, momentum, grads.reshape(2, 128, 4096), hidden)


def solution(mesh):
    in_specs = (
        P(("rep", "fsdp"), None),
        P(),
        P(None, "fsdp", None),
        P(None, "fsdp", None),
        P("rep", None, "fsdp", None),
    )
    out_specs = (P(None, "fsdp", None), P(None, "fsdp", None), P(("rep", "fsdp"), None))
    return jax.shard_map(body, mesh=mesh, in_specs=in_specs, out_specs=out_specs, check_vma=False)
```
